128 devices in a mesh: gx: 4 (over x), gz: 4 (over y_lo, core), ta: 8 (over z, y_hi).
Axes of the slice: x: 4, y: 4 (y_hi: 2, y_lo: 2; y = y_hi * 2 + y_lo), z: 4, core: 2. Of those that a mesh axis runs over, the one named last changes fastest.
Arguments:
- propagator: float32 [2, 12, 12, 1048576], P(None, None, None, ('gx', 'gz', 'ta')), may hold values from -6 to 6
- momenta: int32 [512, 4], P(('gx', 'gz', 'ta')), may hold values from -16 to 15
- gamma_index: int32 [16], replicated, may hold values from 0 to 15, each once
Outputs:
- vertices: float32 [512, 16, 2, 12, 12], P(('gx', 'gz', 'ta'))
The draws below stay inside these ranges and needn't reach their ends.
Inputs may be any that keep to these rules, and one draw needn't show every extreme that they name: `momenta`: A momentum component enters only modulo the lattice length along its direction. `gamma_index`: every mask of 0 to 15 appears once.
All inputs are finite; a program needn't handle non-finite values.
Results may differ from the reference program's by a relative error of at most 0.0001.
Values sent between devices are 32-bit elements; how exact they have to be, the bound alone decides.
A program may use at most 128 MiB of HBM per device.

```python
import jax
import jax.numpy as jnp
import numpy as np
from jax import lax

LX = 32
LY = 32
LZ = 32
LT = 32
SC = 12
NMOM = 512
SITES = 1048576
N_GX = 4
N_GZ = 4
N_TA = 8


def plant(entries, rng, low, high):
    longest = entries.shape.index(max(entries.shape))
    spots = []
    for shift in (0, 1):
        where = [jax.random.randint(jax.random.fold_in(rng, axis), (), 0, length) for axis, length in enumerate(entries.shape)]
        where[longest] = (where[longest] + shift) % entries.shape[longest]
        spots.append(tuple(where))
    return entries.at[spots[0]].set(low).at[spots[1]].set(high)


def level_of(rng, dims, cuts, smallest, largest):
    factor_of, own = 1.0, jax.random.fold_in(rng, 6)
    for position, parts in cuts:
        draws = jnp.exp(jax.random.uniform(jax.random.fold_in(own, position), (parts,), jnp.float32, smallest / len(cuts), largest / len(cuts)))
        factor_of = factor_of * jnp.repeat(draws, dims[position] // parts).reshape([-1 if axis == position else 1 for axis in range(len(dims))])
    return factor_of


def normal_values(stream_key, extent, scale, reach, pieces=(), held_as=jnp.bfloat16):
    level = level_of(stream_key, extent, pieces, -0.22, 0.18) if pieces else 1.0
    result = jax.random.normal(stream_key, extent, jnp.float32) * scale * level
    return jnp.minimum(jnp.maximum(result, -reach), reach).astype(held_as)


def setup_inputs(seed: int = 0) -> dict:
    splits = jax.random.split(jax.random.key(seed), 4)
    return {
        "propagator": normal_values(splits[0], (2, SC, SC, SITES), 1.0, 6.0, ((3, 128),), jnp.float32),
        "momenta": plant(jax.random.randint(splits[1], (NMOM, 4), -16, 16), jax.random.fold_in(splits[1], 1), -16, 15).astype(jnp.int32),
        "gamma_index": jax.random.permutation(splits[2], 16).astype(jnp.int32),
    }


def clifford_table():
    zeros = np.zeros((4, 4))
    first = (zeros, np.array([[0, 0, 0, 1], [0, 0, 1, 0], [0, -1, 0, 0], [-1, 0, 0, 0]]))
    second = (np.array([[0, 0, 0, -1], [0, 0, 1, 0], [0, 1, 0, 0], [-1, 0, 0, 0]]), zeros)
    third = (zeros, np.array([[0, 0, 1, 0], [0, 0, 0, -1], [-1, 0, 0, 0], [0, 1, 0, 0]]))
    fourth = (np.array([[0, 0, 1, 0], [0, 0, 0, 1], [1, 0, 0, 0], [0, 1, 0, 0]]), zeros)
    basis = [first, second, third, fourth]
    tables_re = []
    tables_im = []
    for mask in range(16):
        matrix_re = np.identity(4)
        matrix_im = np.zeros((4, 4))
        for bit in range(4):
            if mask >> bit & 1:
                basis_re, basis_im = basis[bit]
                new_re = matrix_re @ basis_re - matrix_im @ basis_im
                new_im = matrix_re @ basis_im + matrix_im @ basis_re
                matrix_re, matrix_im = (new_re, new_im)
        tables_re.append(matrix_re)
        tables_im.append(matrix_im)
    return (np.stack(tables_re), np.stack(tables_im))

def select_gammas(gamma_index):
    table_re, table_im = clifford_table()
    onehot = (gamma_index[:, None] == jnp.arange(16, dtype=jnp.int32)[None, :]).astype(jnp.float32)
    high = lax.Precision.HIGHEST
    chosen_re = jnp.einsum('gk,kst->gst', onehot, jnp.asarray(table_re, jnp.float32), precision=high)
    chosen_im = jnp.einsum('gk,kst->gst', onehot, jnp.asarray(table_im, jnp.float32), precision=high)
    return (chosen_re, chosen_im)

def vertices_of(spec_re, spec_im, gamma_re, gamma_im):
    high = lax.Precision.HIGHEST
    count = spec_re.shape[0]
    split_re = spec_re.reshape(count, 4, 3, 12)
    split_im = spec_im.reshape(count, 4, 3, 12)
    turned_re = (jnp.einsum('gst,mtcb->mgscb', gamma_re, split_re, precision=high) - jnp.einsum('gst,mtcb->mgscb', gamma_im, split_im, precision=high)).reshape(count, 16, 12, 12)
    turned_im = (jnp.einsum('gst,mtcb->mgscb', gamma_re, split_im, precision=high) + jnp.einsum('gst,mtcb->mgscb', gamma_im, split_re, precision=high)).reshape(count, 16, 12, 12)
    result_re = jnp.einsum('mka,mgkb->mgab', spec_re, turned_re, precision=high) + jnp.einsum('mka,mgkb->mgab', spec_im, turned_im, precision=high)
    result_im = jnp.einsum('mka,mgkb->mgab', spec_re, turned_im, precision=high) - jnp.einsum('mka,mgkb->mgab', spec_im, turned_re, precision=high)
    return jnp.stack([result_re, result_im], axis=2)

def reference(propagator, momenta, gamma_index):
    block_x = LX // N_GX
    block_z = LZ // N_GZ
    block_t = LT // N_TA
    field = propagator.reshape(2, 12, 12, N_GX, N_GZ, N_TA, block_x, LY, block_z, block_t)
    field = jnp.transpose(field, (0, 1, 2, 3, 6, 7, 4, 8, 5, 9)).reshape(2, 12, 12, LX, LY, LZ, LT)
    complex_field = lax.complex(field[0], field[1])
    spectrum_all = jnp.fft.fftn(complex_field, axes=(2, 3, 4, 5))
    index_x = (momenta[:, 0] % LX).astype(jnp.int32)
    index_y = (momenta[:, 1] % LY).astype(jnp.int32)
    index_z = (momenta[:, 2] % LZ).astype(jnp.int32)
    index_t = (momenta[:, 3] % LT).astype(jnp.int32)
    picked = spectrum_all[:, :, index_x, index_y, index_z, index_t]
    picked = jnp.transpose(picked, (2, 0, 1))
    scale = 1.0 / np.sqrt(float(SITES))
    spec_re = (jnp.real(picked) * scale).astype(jnp.float32)
    spec_im = (jnp.imag(picked) * scale).astype(jnp.float32)
    gamma_re, gamma_im = select_gammas(gamma_index)
    return vertices_of(spec_re, spec_im, gamma_re, gamma_im)
```

```python
import functools
import math

import jax
import jax.numpy as jnp
import numpy as np
from jax import lax
from jax.experimental import pallas as pl
from jax.experimental.pallas import tpu as pltpu
from jax.sharding import PartitionSpec as P

LX = LY = LZ = LT = 32
MESH = pl.DeviceIdType.MESH
F32 = jnp.float32
BF16 = jnp.bfloat16
TILES = 11
CHUNKS = 9
ROWS = 384


def fold_matrices():
    out = np.zeros((8, 2, 8, 8, 8, 2))
    for q in range(8):
        r = 2 * q if q < 4 else 2 * (q - 4) + 1
        for h in range(8):
            w = np.exp(-2j * np.pi * r * h / 8)
            for x in range(8):
                out[q, 0, x, x, h, 0] = w.real
                out[q, 0, x, x, h, 1] = -w.imag
                out[q, 1, x, x, h, 0] = w.imag
                out[q, 1, x, x, h, 1] = w.real
    full = out.reshape(128, 128).astype(np.float32)
    high = full.astype(jnp.bfloat16)
    low = (full - high.astype(np.float32)).astype(jnp.bfloat16)
    return np.concatenate([high, high], 1), np.concatenate([low, 0 * low], 1)[64:]


def split(value):
    high = value.astype(BF16)
    return high, (value - high.astype(F32)).astype(BF16)


def sine(index):
    turn = ((index + 16) & 31) - 16
    turn = jnp.where(turn > 8, 16 - turn, jnp.where(turn < -8, -16 - turn, turn))
    u = turn.astype(F32) * (math.pi / 16)
    s = u * u
    poly = 1 / 362880 - s * (1 / 39916800)
    for factor in (-1 / 5040, 1 / 120, -1 / 6, 1.0):
        poly = factor + s * poly
    return u * poly


def wave(index):
    return sine(index + 8), -sine(index)


def sum_over_x(value):
    groups = value.shape[0] // 8
    value = value.reshape(groups, 8, 8, 128)
    sub = lax.broadcasted_iota(jnp.int32, (8, 128), 0)
    for step in (4, 2, 1):
        keep = (sub & step) == 0
        out = []
        for k in range(step):
            a, b = value[:, k], value[:, k + step]
            rolled_a = pltpu.roll(a, 8 - step, 1)
            rolled_b = pltpu.roll(b, step, 1)
            out.append(jnp.where(keep, a, rolled_b) + jnp.where(keep, rolled_a, b))
        value = jnp.stack(out, axis=1)
    return value.reshape(groups * 8, 128)


NT = (((1,), (1,)), ((), ()))


def iota(shape, dim):
    return lax.broadcasted_iota(jnp.int32, shape, dim)


def compute_kernel(
    row_order, x_hbm, mom_ref, fold_ref, fold_low_ref, z_ref, sbuf, gh, gl, yall, pick, sems
):
    copies = []
    for k in range(CHUNKS):
        part = pl.ds(k * 16, 16)
        copies.append(pltpu.make_async_copy(x_hbm.at[part], sbuf.at[part], sems.at[k]))
        copies[-1].start()
    gx, gz, ta = (lax.axis_index(name) for name in ("gx", "gz", "ta"))

    for k in range(CHUNKS):
        copies[k].wait()

        def pair_step(p, carry, k=k):
            pair = k * 8 + p
            both = jnp.concatenate([sbuf[2 * pair], sbuf[2 * pair + 1]], axis=1)
            weights = jnp.concatenate(split(both), axis=0)
            out = jnp.dot(fold_ref[...], weights, preferred_element_type=F32)
            low = jnp.dot(fold_low_ref[...], weights, preferred_element_type=F32)
            out = jnp.concatenate([out[:64], out[64:] + low], axis=0)
            left = out[:, :128].reshape(16, 8, 128)
            right = out[:, 128:].reshape(16, 8, 128)
            high, rest = split(jnp.concatenate([left, right], axis=1))
            rows = pl.ds(pl.multiple_of(pair * 16, 16), 16)
            for q in range(8):
                for part in range(2):
                    lanes = slice(part * 128, part * 128 + 128)
                    gh[q, rows, lanes] = high[2 * q + part]
                    gl[q, rows, lanes] = rest[2 * q + part]
            return carry

        lax.fori_loop(0, 8, pair_step, 0)

    turned = jnp.transpose((mom_ref[...] & 31).astype(F32))
    mom = jnp.concatenate([turned[4 * i : 4 * i + 4] for i in range(4)], axis=1)
    ny = mom[1:2].astype(jnp.int32)
    cls = ((ny >> 1) & 3) + 4 * (ny & 1)
    member = (iota((8, 512), 0) == cls).astype(F32)
    before = (iota((512, 512), 0) < iota((512, 512), 1)).astype(F32).astype(BF16)
    ahead = jnp.dot(member.astype(BF16), before, preferred_element_type=F32)
    slot = jnp.sum(member * ahead, axis=0, keepdims=True)
    ends = []
    start = jnp.int32(0)
    for q in range(8):
        count = jnp.sum(member[q : q + 1]).astype(jnp.int32)
        slot = slot + member[q : q + 1] * (start * 128).astype(F32)
        start = start + ((count + 127) >> 7)
        ends.append(start)
    slot = slot.astype(jnp.int32)
    mom8 = jnp.concatenate([mom, jnp.zeros_like(mom)], axis=0).astype(BF16)
    digits = jnp.concatenate([slot >> 5, slot & 31] + [slot * 0] * 6, axis=0).astype(F32).astype(BF16)
    source = row_order(iota((512, 512), 0))
    move = (source == iota((512, 512), 1)).astype(F32).astype(BF16)
    column = lax.dot_general(move, digits, NT, preferred_element_type=F32)
    column = (column[:, 0:1] * 32.0 + column[:, 1:2]).astype(jnp.int32)

    def tile_step(j, carry):
        q = jnp.int32(0)
        for end in ends[:7]:
            q = q + (end <= j).astype(jnp.int32)
        here = (iota((128, 512), 0) + j * 128 == slot).astype(F32).astype(BF16)
        sorted_mom = lax.dot_general(mom8, here, NT, preferred_element_type=F32).astype(jnp.int32)
        nx, ny, nz, nt = (sorted_mom[i : i + 1] for i in range(4))
        site = iota((128, 128), 0)
        pr, pi = wave(ny * (site >> 5) + nz * ((site >> 2) & 7) + nt * (site & 3))
        (prh, prl), (pih, pil) = split(pr), split(pi)
        w_high = jnp.concatenate(
            [jnp.concatenate([prh, pih], 1), jnp.concatenate([-pih, prh], 1)], 0
        )
        w_low = jnp.concatenate(
            [jnp.concatenate([prl, pil], 1), jnp.concatenate([-pil, prl], 1)], 0
        )
        xr, xi = wave(nx * (gx * 8 + iota((8, 128), 0)) + nz * (gz * 8) + nt * (ta * 4))
        lanes = pl.ds(pl.multiple_of(j * 256, 256), 128)
        lanes_low = pl.ds(pl.multiple_of(j * 256 + 128, 128), 128)
        for c in range(1152 // ROWS):
            rows = pl.ds(c * ROWS, ROWS)
            high = gh[q, rows]
            out = (
                jnp.dot(high, w_high, preferred_element_type=F32)
                + jnp.dot(gl[q, rows], w_high, preferred_element_type=F32)
                + jnp.dot(high, w_low, preferred_element_type=F32)
            )
            re = out[:, :128].reshape(ROWS // 8, 8, 128)
            im = out[:, 128:].reshape(ROWS // 8, 8, 128)
            for part, value in enumerate((re * xr - im * xi, re * xi + im * xr)):
                top, rest = split(sum_over_x(value))
                to = pl.ds(part * 144 + c * (ROWS // 8), ROWS // 8)
                yall[to, lanes] = top
                yall[to, lanes_low] = rest
        chosen = (iota((512, 128), 1) + j * 128 == column).astype(F32).astype(BF16)
        pick[:, lanes] = chosen
        pick[:, lanes_low] = chosen
        return carry

    lax.fori_loop(0, TILES, tile_step, 0)
    z_ref[...] = lax.dot_general(pick[...], yall[...], NT, preferred_element_type=F32)


def partial_spectrum(x, mom, row_order):
    fold, fold_low = fold_matrices()
    vmem = pl.BlockSpec(memory_space=pltpu.VMEM)
    return pl.pallas_call(
        functools.partial(compute_kernel, row_order),
        out_shape=jax.ShapeDtypeStruct((512, 288), F32),
        in_specs=[pl.BlockSpec(memory_space=pl.ANY), vmem, vmem, vmem],
        out_specs=vmem,
        scratch_shapes=[
            pltpu.VMEM((144, 128, 128), F32),
            pltpu.VMEM((8, 1152, 256), BF16),
            pltpu.VMEM((8, 1152, 256), BF16),
            pltpu.VMEM((288, TILES * 256), BF16),
            pltpu.VMEM((512, TILES * 256), BF16),
            pltpu.SemaphoreType.DMA((CHUNKS,)),
        ],
        compiler_params=pltpu.CompilerParams(vmem_limit_bytes=50 * 1024 * 1024),
    )(x, mom, jnp.asarray(fold), jnp.asarray(fold_low))


def gather_kernel(sizes, row_ref, out_ref, send_sem, recv_sem):
    n_gx, n_gz, n_ta = sizes
    total = n_gx * n_gz * n_ta
    me = (lax.axis_index("gx") * n_gz + lax.axis_index("gz")) * n_ta + lax.axis_index("ta")

    def device(k):
        peer = lax.rem(me + k, total)
        return (peer // (n_gz * n_ta), lax.rem(peer // n_ta, n_gz), lax.rem(peer, n_ta))

    barrier = pltpu.get_barrier_semaphore()

    def greet(k, carry):
        pl.semaphore_signal(barrier, inc=1, device_id=device(k), device_id_type=MESH)
        return carry

    lax.fori_loop(1, total, greet, 0)
    out_ref[me] = row_ref[...]
    pl.semaphore_wait(barrier, total - 1)

    def copy(k):
        return pltpu.make_async_remote_copy(
            src_ref=row_ref,
            dst_ref=out_ref.at[me],
            send_sem=send_sem,
            recv_sem=recv_sem,
            device_id=device(k),
            device_id_type=MESH,
        )

    def send(k, carry):
        copy(k).start()
        return carry

    lax.fori_loop(1, total, send, 0)
    everything = out_ref.at[pl.ds(0, total - 1)]
    pltpu.make_async_copy(everything, everything, send_sem).wait()
    pltpu.make_async_copy(everything, everything, recv_sem).wait()


def gather_momenta(momenta, sizes):
    total = math.prod(sizes)
    row = jnp.pad(momenta.reshape(1, 16), ((0, 0), (0, 112)))
    vmem = pl.BlockSpec(memory_space=pltpu.VMEM)
    out = pl.pallas_call(
        functools.partial(gather_kernel, sizes),
        out_shape=jax.ShapeDtypeStruct((total, 1, 128), jnp.int32),
        in_specs=[vmem],
        out_specs=vmem,
        scratch_shapes=[pltpu.SemaphoreType.DMA, pltpu.SemaphoreType.DMA],
        compiler_params=pltpu.CompilerParams(collective_id=0, has_side_effects=True),
    )(row)
    return out.reshape(total, 128)


def in_blocks(array, dim, devices):
    before, after = (array.shape[:dim], array.shape[dim + 1 :])
    return jnp.moveaxis(array.reshape(*before, devices, -1, *after), dim, 0)


def summed_on_arrival(array, axis, dim):
    devices = lax.axis_size(axis)
    blocks = lax.all_to_all(in_blocks(array, dim, devices), axis, 0, 0, tiled=True)
    return jnp.sum(blocks, axis=0)


def clifford_table():
    zeros = np.zeros((4, 4))
    first = (zeros, np.array([[0, 0, 0, 1], [0, 0, 1, 0], [0, -1, 0, 0], [-1, 0, 0, 0]]))
    second = (np.array([[0, 0, 0, -1], [0, 0, 1, 0], [0, 1, 0, 0], [-1, 0, 0, 0]]), zeros)
    third = (zeros, np.array([[0, 0, 1, 0], [0, 0, 0, -1], [-1, 0, 0, 0], [0, 1, 0, 0]]))
    fourth = (np.array([[0, 0, 1, 0], [0, 0, 0, 1], [1, 0, 0, 0], [0, 1, 0, 0]]), zeros)
    basis = [first, second, third, fourth]
    tables_re = []
    tables_im = []
    for mask in range(16):
        matrix_re = np.identity(4)
        matrix_im = np.zeros((4, 4))
        for bit in range(4):
            if mask >> bit & 1:
                basis_re, basis_im = basis[bit]
                new_re = matrix_re @ basis_re - matrix_im @ basis_im
                new_im = matrix_re @ basis_im + matrix_im @ basis_re
                matrix_re, matrix_im = (new_re, new_im)
        tables_re.append(matrix_re)
        tables_im.append(matrix_im)
    return (np.stack(tables_re), np.stack(tables_im))


def select_gammas(gamma_index):
    table_re, table_im = clifford_table()
    onehot = (gamma_index[:, None] == jnp.arange(16, dtype=jnp.int32)[None, :]).astype(jnp.float32)
    high = lax.Precision.HIGHEST
    chosen_re = jnp.einsum(
        "gk,kst->gst", onehot, jnp.asarray(table_re, jnp.float32), precision=high
    )
    chosen_im = jnp.einsum(
        "gk,kst->gst", onehot, jnp.asarray(table_im, jnp.float32), precision=high
    )
    return (chosen_re, chosen_im)


def vertices_of(spec_re, spec_im, gamma_re, gamma_im):
    high = lax.Precision.HIGHEST
    count = spec_re.shape[0]
    split_re = spec_re.reshape(count, 4, 3, 12)
    split_im = spec_im.reshape(count, 4, 3, 12)
    turned_re = (
        jnp.einsum("gst,mtcb->mgscb", gamma_re, split_re, precision=high)
        - jnp.einsum("gst,mtcb->mgscb", gamma_im, split_im, precision=high)
    ).reshape(count, 16, 12, 12)
    turned_im = (
        jnp.einsum("gst,mtcb->mgscb", gamma_re, split_im, precision=high)
        + jnp.einsum("gst,mtcb->mgscb", gamma_im, split_re, precision=high)
    ).reshape(count, 16, 12, 12)
    result_re = jnp.einsum("mka,mgkb->mgab", spec_re, turned_re, precision=high) + jnp.einsum(
        "mka,mgkb->mgab", spec_im, turned_im, precision=high
    )
    result_im = jnp.einsum("mka,mgkb->mgab", spec_re, turned_im, precision=high) - jnp.einsum(
        "mka,mgkb->mgab", spec_im, turned_re, precision=high
    )
    return jnp.stack([result_re, result_im], axis=2)


def site_major(propagator):
    x = jnp.transpose(propagator, (1, 2, 0, 3)).reshape(144, 2, 64, 128)
    return jnp.transpose(x, (0, 2, 1, 3)).reshape(144, 128, 128)


def body(sizes, propagator, momenta, gamma_index):
    mine = momenta.shape[0]
    total = math.prod(sizes)
    n_ta = sizes[2]
    gathered = gather_momenta(momenta, sizes)

    def row_order(row):
        ta, spatial, own = row // (total // n_ta * mine), row // mine % (total // n_ta), row % mine
        return own * total + spatial * n_ta + ta

    partial_value = partial_spectrum(site_major(propagator), gathered, row_order)
    partial_value = summed_on_arrival(partial_value, "ta", 0)
    spectrum = summed_on_arrival(partial_value, ("gx", "gz"), 0)
    spectrum = spectrum * (1.0 / math.sqrt(float(LX * LY * LZ * LT)))
    spectrum = spectrum.reshape(mine, 2, 12, 12)
    gamma_re, gamma_im = select_gammas(gamma_index)
    return vertices_of(spectrum[:, 0], spectrum[:, 1], gamma_re, gamma_im)


def solution(mesh):
    placed = (P(None, None, None, ("gx", "gz", "ta")), P(("gx", "gz", "ta"), None), P())
    sizes = tuple(mesh.shape[name] for name in ("gx", "gz", "ta"))
    return jax.shard_map(
        functools.partial(body, sizes),
        mesh=mesh,
        in_specs=placed,
        out_specs=P(("gx", "gz", "ta"), None, None, None, None),
        check_vma=False,
    )
```

```python
import math

import jax
import jax.numpy as jnp
import numpy as np
from jax import lax
from jax.experimental import pallas as pl
from jax.experimental.pallas import tpu as pltpu
from jax.sharding import PartitionSpec as P

LX = LY = LZ = LT = 32
MESH = pl.DeviceIdType.MESH
F32 = jnp.float32
BF16 = jnp.bfloat16
TILES = 11
CHUNKS = 18
HALF = 72


def split(value):
    high = value.astype(BF16)
    return high, (value - high.astype(F32)).astype(BF16)


def sine(index):
    turn = ((index + 16) & 31) - 16
    turn = jnp.where(turn > 8, 16 - turn, jnp.where(turn < -8, -16 - turn, turn))
    u = turn.astype(F32) * (math.pi / 16)
    s = u * u
    poly = 1 / 362880 - s * (1 / 39916800)
    for factor in (-1 / 5040, 1 / 120, -1 / 6, 1.0):
        poly = factor + s * poly
    return u * poly


def wave(index):
    return sine(index + 8), -sine(index)


def sum_over_x(value):
    groups = value.shape[0] // 8
    value = value.reshape(groups, 8, 8, 128)
    sub = lax.broadcasted_iota(jnp.int32, (8, 128), 0)
    for step in (4, 2, 1):
        keep = (sub & step) == 0
        out = []
        for k in range(step):
            a, b = value[:, k], value[:, k + step]
            rolled_a = pltpu.roll(a, 8 - step, 1)
            rolled_b = pltpu.roll(b, step, 1)
            out.append(jnp.where(keep, a, rolled_b) + jnp.where(keep, rolled_a, b))
        value = jnp.stack(out, axis=1)
    return value.reshape(groups * 8, 128)


NT = (((1,), (1,)), ((), ()))


def iota(shape, dim):
    return lax.broadcasted_iota(jnp.int32, shape, dim)


def fold_matrix():
    row, col = iota((128, 128), 0), iota((128, 128), 1)
    q = row >> 4
    number = jnp.where(q < 4, 2 * q, 2 * q - 7)
    re, im = wave(4 * number * ((col >> 1) & 7))
    from_im, to_im = (col & 1) == 1, ((row >> 3) & 1) == 1
    value = jnp.where(from_im == to_im, re, jnp.where(to_im, im, -im))
    return split(jnp.where((row & 7) == (col >> 4), value, 0.0))


def program_kernel(
    x_hbm, mom_smem, out_ref,
    sbuf, gh, gl, w_high, w_low, x_wave, yall, pick, row_buf, mom_all,
    zbuf, dbuf, hbuf, rbuf, spec,
    in_sems, mom_send, mom_recv, pair_send, pair_recv, far_send, far_recv, last_send, last_recv,
):
    gx, gz, ta = (lax.axis_index(name) for name in ("gx", "gz", "ta"))
    core, y_lo, z, y_hi = gz % 2, gz // 2, ta // 2, ta % 2
    y = y_hi * 2 + y_lo
    me = (gx * 4 + gz) * 8 + ta
    chip = (gx * 2 + y_lo) * 8 + ta
    xs = [gx] + [(gx + k) % 4 for k in range(1, 4)]
    ys = [y] + [(y + k) % 4 for k in range(1, 4)]
    zs = [z] + [(z + k) % 4 for k in range(1, 4)]
    cores = [core, 1 - core]
    gzs = [[(value % 2) * 2 + c for c in cores] for value in ys]
    tas = [[at_z * 2 + value // 2 for at_z in zs] for value in ys]
    hops = (0, 1, 2, 1)
    chips = sorted(
        ((dx, dy, dz) for dx in range(4) for dy in range(4) for dz in range(4)),
        key=lambda d: -sum(hops[k] for k in d),
    )

    def device(place, dc=0):
        dx, dy, dz = place
        return (xs[dx], gzs[dy][dc], tas[dy][dz])

    def chip_of(place):
        dx, dy, dz = place
        return (xs[dx] * 2 + ys[dy] % 2) * 8 + tas[dy][dz]

    others = [(place, dc) for place in chips for dc in (0, 1) if place != (0, 0, 0) or dc]
    barrier = pltpu.get_barrier_semaphore()
    for place, dc in others:
        pl.semaphore_signal(barrier, inc=1, device_id=device(place, dc), device_id_type=MESH)

    def load(k):
        part = pl.ds(k * 8, 8)
        return pltpu.make_async_copy(x_hbm.at[part], sbuf.at[part], in_sems.at[k])

    for k in range(CHUNKS):
        load(k).start()
    row = jnp.zeros((1, 128), jnp.int32)
    for i in range(4):
        for k in range(4):
            row = jnp.where(iota((1, 128), 1) == 4 * i + k, mom_smem[i, k], row)
    row_buf[...] = row
    mom_all[me] = row

    fold_high, fold_low = fold_matrix()
    fold_twice = jnp.concatenate([fold_high, fold_high], axis=1)
    fold_rest = jnp.concatenate([fold_low, jnp.zeros_like(fold_low)], axis=1)[64:]

    def fold_step(k, carry):
        load(k).wait()
        for p in range(4):
            pair = k * 4 + p
            both = jnp.concatenate([sbuf[2 * pair], sbuf[2 * pair + 1]], axis=1)
            weights = jnp.concatenate(split(both), axis=0)
            out = jnp.dot(fold_twice, weights, preferred_element_type=F32)
            low = jnp.dot(fold_rest, weights, preferred_element_type=F32)
            out = jnp.concatenate([out[:64], out[64:] + low], axis=0)
            left = out[:, :128].reshape(16, 8, 128)
            right = out[:, 128:].reshape(16, 8, 128)
            high, rest = split(jnp.concatenate([left, right], axis=1))
            rows = pl.ds(pl.multiple_of(pair * 16, 16), 16)
            for q in range(8):
                for part in range(2):
                    lanes = slice(part * 128, part * 128 + 128)
                    gh[q, rows, lanes] = high[2 * q + part]
                    gl[q, rows, lanes] = rest[2 * q + part]
        return carry

    lax.fori_loop(0, CHUNKS // 2, fold_step, 0)

    pl.semaphore_wait(barrier, 127)
    for place, dc in others:
        pltpu.make_async_remote_copy(
            src_ref=row_buf, dst_ref=mom_all.at[me], send_sem=mom_send, recv_sem=mom_recv,
            device_id=device(place, dc), device_id_type=MESH,
        ).start()

    lax.fori_loop(CHUNKS // 2, CHUNKS, fold_step, 0)

    all_rows = mom_all.at[pl.ds(0, 127)]
    pltpu.make_async_copy(all_rows, all_rows, mom_recv).wait()

    turned = jnp.transpose((mom_all[...].reshape(128, 128) & 31).astype(F32))
    mom = jnp.concatenate([turned[4 * i : 4 * i + 4] for i in range(4)], axis=1)
    ny = mom[1:2].astype(jnp.int32)
    cls = ((ny >> 1) & 3) + 4 * (ny & 1)
    member = (iota((8, 512), 0) == cls).astype(F32)
    before = (iota((512, 512), 0) < iota((512, 512), 1)).astype(F32).astype(BF16)
    ahead = jnp.dot(member.astype(BF16), before, preferred_element_type=F32)
    slot = jnp.sum(member * ahead, axis=0, keepdims=True)
    ends = []
    start = jnp.int32(0)
    for q in range(8):
        count = jnp.sum(member[q : q + 1]).astype(jnp.int32)
        slot = slot + member[q : q + 1] * (start * 128).astype(F32)
        start = start + ((count + 127) >> 7)
        ends.append(start)
    slot = slot.astype(jnp.int32)
    mom8 = jnp.concatenate([mom, jnp.zeros_like(mom)], axis=0).astype(BF16)
    digits = jnp.concatenate([slot >> 5, slot & 31] + [slot * 0] * 6, axis=0).astype(F32).astype(BF16)
    to_row = iota((512, 512), 0)
    to_chip, to_core, own = to_row >> 3, (to_row >> 2) & 1, to_row & 3
    source = own * 128 + ((to_chip >> 3) * 2 + to_core) * 8 + (to_chip & 7)
    move = (source == iota((512, 512), 1)).astype(F32).astype(BF16)
    column = lax.dot_general(move, digits, NT, preferred_element_type=F32)
    column = (column[:, 0:1] * 32.0 + column[:, 1:2]).astype(jnp.int32)

    def prepare(j):
        here = (iota((128, 512), 0) + j * 128 == slot).astype(F32).astype(BF16)
        sorted_mom = lax.dot_general(mom8, here, NT, preferred_element_type=F32).astype(jnp.int32)
        nx, ny, nz, nt = (sorted_mom[i : i + 1] for i in range(4))
        site = iota((128, 128), 0)
        pr, pi = wave(ny * (site >> 5) + nz * ((site >> 2) & 7) + nt * (site & 3))
        (prh, prl), (pih, pil) = split(pr), split(pi)
        w_high[j] = jnp.concatenate(
            [jnp.concatenate([prh, pih], 1), jnp.concatenate([-pih, prh], 1)], 0
        )
        w_low[j] = jnp.concatenate(
            [jnp.concatenate([prl, pil], 1), jnp.concatenate([-pil, prl], 1)], 0
        )
        xr, xi = wave(nx * (gx * 8 + iota((8, 128), 0)) + nz * (gz * 8) + nt * (ta * 4))
        x_wave[j, 0] = xr
        x_wave[j, 1] = xi

    def multiply(j, half):
        q = jnp.int32(0)
        for end in ends[:7]:
            q = q + (end <= j).astype(jnp.int32)
        rows = pl.ds(half * HALF * 8, HALF * 8)
        high = gh[q, rows]
        top = w_high[j]
        out = (
            jnp.dot(high, top, preferred_element_type=F32)
            + jnp.dot(gl[q, rows], top, preferred_element_type=F32)
            + jnp.dot(high, w_low[j], preferred_element_type=F32)
        )
        xr, xi = x_wave[j, 0], x_wave[j, 1]
        re = out[:, :128].reshape(HALF, 8, 128)
        im = out[:, 128:].reshape(HALF, 8, 128)
        lanes = pl.ds(pl.multiple_of(j * 256, 256), 128)
        lanes_low = pl.ds(pl.multiple_of(j * 256 + 128, 128), 128)
        for part, value in enumerate((re * xr - im * xi, re * xi + im * xr)):
            first, rest = split(sum_over_x(value))
            to = pl.ds(part * 128, HALF)
            yall[half, to, lanes] = first
            yall[half, to, lanes_low] = rest

    def choose(j):
        lanes = pl.ds(pl.multiple_of(j * 256, 256), 128)
        lanes_low = pl.ds(pl.multiple_of(j * 256 + 128, 128), 128)
        chosen = (iota((512, 128), 1) + j * 128 == column).astype(F32).astype(BF16)
        pick[:, lanes] = chosen
        pick[:, lanes_low] = chosen

    def first_step(j, carry):
        multiply(j, 0)
        prepare(j + 1)
        choose(j)
        return carry

    def second_step(j, carry):
        multiply(j, 1)
        return carry

    def to_partner(half):
        return pltpu.make_async_remote_copy(
            src_ref=zbuf.at[half, 1 - core], dst_ref=dbuf.at[half],
            send_sem=pair_send.at[half], recv_sem=pair_recv.at[half],
            device_id=device((0, 0, 0), 1), device_id_type=MESH,
        )

    def restore(half):
        back = lax.dot_general(pick[...], yall[half], NT, preferred_element_type=F32)
        zbuf[half, 0] = back[:, :128]
        zbuf[half, 1] = back[:, 128:]
        to_partner(half).start()

    def send_far(half):
        to_partner(half).wait_recv()
        total = (zbuf[half, core] + dbuf[half]) * (1.0 / math.sqrt(float(LX * LY * LZ * LT)))
        hbuf[half] = total.reshape(64, 8, 128)
        rbuf[half, chip] = hbuf[half, chip]
        for place in chips[:-1]:
            pltpu.make_async_remote_copy(
                src_ref=hbuf.at[half, chip_of(place)], dst_ref=rbuf.at[half, chip],
                send_sem=far_send.at[half], recv_sem=far_recv.at[half],
                device_id=device(place), device_id_type=MESH,
            ).start()

    def wait_far(half):
        blocks = rbuf.at[half, pl.ds(0, 63)]
        pltpu.make_async_copy(blocks, blocks, far_recv.at[half]).wait()
        spec[core, half] = jnp.sum(rbuf[half], axis=0)

    prepare(jnp.int32(0))
    lax.fori_loop(0, TILES, first_step, 0)
    restore(0)
    lax.fori_loop(0, TILES // 2, second_step, 0)
    send_far(0)
    lax.fori_loop(TILES // 2, TILES, second_step, 0)
    restore(1)
    send_far(1)
    wait_far(0)
    wait_far(1)
    last = pltpu.make_async_remote_copy(
        src_ref=spec.at[core], dst_ref=spec.at[core], send_sem=last_send, recv_sem=last_recv,
        device_id=device((0, 0, 0), 1), device_id_type=MESH,
    )
    last.start()
    pltpu.make_async_copy(all_rows, all_rows, mom_send).wait()
    for half in range(2):
        to_partner(half).wait_send()
        blocks = hbuf.at[half, pl.ds(0, 63)]
        pltpu.make_async_copy(blocks, blocks, far_send.at[half]).wait()
    last.wait()
    value = spec[...]
    out_ref[...] = jnp.where(core == 0, value[:, :, :4], value[:, :, 4:])


def spectrum_of(x, momenta):
    vmem = pl.BlockSpec(memory_space=pltpu.VMEM)
    dma = pltpu.SemaphoreType.DMA
    return pl.pallas_call(
        program_kernel,
        out_shape=jax.ShapeDtypeStruct((2, 2, 4, 128), F32),
        in_specs=[pl.BlockSpec(memory_space=pl.ANY), pl.BlockSpec(memory_space=pltpu.SMEM)],
        out_specs=vmem,
        scratch_shapes=[
            pltpu.VMEM((144, 128, 128), F32),
            pltpu.VMEM((8, 1152, 256), BF16),
            pltpu.VMEM((8, 1152, 256), BF16),
            pltpu.VMEM((TILES + 1, 256, 256), BF16),
            pltpu.VMEM((TILES + 1, 256, 256), BF16),
            pltpu.VMEM((TILES + 1, 2, 8, 128), F32),
            pltpu.VMEM((2, 256, TILES * 256), BF16),
            pltpu.VMEM((512, TILES * 256), BF16),
            pltpu.VMEM((1, 128), jnp.int32),
            pltpu.VMEM((128, 1, 128), jnp.int32),
            pltpu.VMEM((2, 2, 512, 128), F32),
            pltpu.VMEM((2, 512, 128), F32),
            pltpu.VMEM((2, 64, 8, 128), F32),
            pltpu.VMEM((2, 64, 8, 128), F32),
            pltpu.VMEM((2, 2, 8, 128), F32),
            dma((CHUNKS,)),
            dma, dma, dma((2,)), dma((2,)), dma((2,)), dma((2,)), dma, dma,
        ],
        compiler_params=pltpu.CompilerParams(
            collective_id=0, has_side_effects=True, vmem_limit_bytes=56 * 1024 * 1024
        ),
    )(x, momenta)


def clifford_table():
    zeros = np.zeros((4, 4))
    first = (zeros, np.array([[0, 0, 0, 1], [0, 0, 1, 0], [0, -1, 0, 0], [-1, 0, 0, 0]]))
    second = (np.array([[0, 0, 0, -1], [0, 0, 1, 0], [0, 1, 0, 0], [-1, 0, 0, 0]]), zeros)
    third = (zeros, np.array([[0, 0, 1, 0], [0, 0, 0, -1], [-1, 0, 0, 0], [0, 1, 0, 0]]))
    fourth = (np.array([[0, 0, 1, 0], [0, 0, 0, 1], [1, 0, 0, 0], [0, 1, 0, 0]]), zeros)
    basis = [first, second, third, fourth]
    tables_re = []
    tables_im = []
    for mask in range(16):
        matrix_re = np.identity(4)
        matrix_im = np.zeros((4, 4))
        for bit in range(4):
            if mask >> bit & 1:
                basis_re, basis_im = basis[bit]
                new_re = matrix_re @ basis_re - matrix_im @ basis_im
                new_im = matrix_re @ basis_im + matrix_im @ basis_re
                matrix_re, matrix_im = (new_re, new_im)
        tables_re.append(matrix_re)
        tables_im.append(matrix_im)
    return (np.stack(tables_re), np.stack(tables_im))


def select_gammas(gamma_index):
    table_re, table_im = clifford_table()
    onehot = (gamma_index[:, None] == jnp.arange(16, dtype=jnp.int32)[None, :]).astype(jnp.float32)
    high = lax.Precision.HIGHEST
    chosen_re = jnp.einsum(
        "gk,kst->gst", onehot, jnp.asarray(table_re, jnp.float32), precision=high
    )
    chosen_im = jnp.einsum(
        "gk,kst->gst", onehot, jnp.asarray(table_im, jnp.float32), precision=high
    )
    return (chosen_re, chosen_im)


def vertices_of(spec_re, spec_im, gamma_re, gamma_im):
    high = lax.Precision.HIGHEST
    count = spec_re.shape[0]
    split_re = spec_re.reshape(count, 4, 3, 12)
    split_im = spec_im.reshape(count, 4, 3, 12)
    turned_re = (
        jnp.einsum("gst,mtcb->mgscb", gamma_re, split_re, precision=high)
        - jnp.einsum("gst,mtcb->mgscb", gamma_im, split_im, precision=high)
    ).reshape(count, 16, 12, 12)
    turned_im = (
        jnp.einsum("gst,mtcb->mgscb", gamma_re, split_im, precision=high)
        + jnp.einsum("gst,mtcb->mgscb", gamma_im, split_re, precision=high)
    ).reshape(count, 16, 12, 12)
    result_re = jnp.einsum("mka,mgkb->mgab", spec_re, turned_re, precision=high) + jnp.einsum(
        "mka,mgkb->mgab", spec_im, turned_im, precision=high
    )
    result_im = jnp.einsum("mka,mgkb->mgab", spec_re, turned_im, precision=high) - jnp.einsum(
        "mka,mgkb->mgab", spec_im, turned_re, precision=high
    )
    return jnp.stack([result_re, result_im], axis=2)


def site_major(propagator):
    x = jnp.transpose(propagator, (1, 2, 0, 3)).reshape(144, 2, 64, 128)
    return jnp.transpose(x, (0, 2, 1, 3)).reshape(144, 128, 128)


def body(propagator, momenta, gamma_index):
    spectrum = spectrum_of(site_major(propagator), momenta)[:, :, :, :HALF]
    spectrum = jnp.transpose(spectrum, (2, 0, 1, 3)).reshape(4, 2, 12, 12)
    gamma_re, gamma_im = select_gammas(gamma_index)
    return vertices_of(spectrum[:, 0], spectrum[:, 1], gamma_re, gamma_im)


def solution(mesh):
    placed = (P(None, None, None, ("gx", "gz", "ta")), P(("gx", "gz", "ta"), None), P())
    return jax.shard_map(
        body,
        mesh=mesh,
        in_specs=placed,
        out_specs=P(("gx", "gz", "ta"), None, None, None, None),
        check_vma=False,
    )
```

```python
import math

import jax
import jax.numpy as jnp
import numpy as np
from jax import lax
from jax.experimental import pallas as pl
from jax.experimental.pallas import tpu as pltpu
from jax.sharding import PartitionSpec as P

LX = LY = LZ = LT = 32
MESH = pl.DeviceIdType.MESH
F32 = jnp.float32
BF16 = jnp.bfloat16
TILES = 11
CHUNKS = 18
HALF = 72


def split(value):
    high = value.astype(BF16)
    return high, (value - high.astype(F32)).astype(BF16)


def sine(index):
    turn = ((index + 16) & 31) - 16
    turn = jnp.where(turn > 8, 16 - turn, jnp.where(turn < -8, -16 - turn, turn))
    u = turn.astype(F32) * (math.pi / 16)
    s = u * u
    poly = 1 / 362880 - s * (1 / 39916800)
    for factor in (-1 / 5040, 1 / 120, -1 / 6, 1.0):
        poly = factor + s * poly
    return u * poly


def wave(index):
    return sine(index + 8), -sine(index)


def sum_over_x(value):
    groups = value.shape[0] // 8
    value = value.reshape(groups, 8, 8, 128)
    sub = lax.broadcasted_iota(jnp.int32, (8, 128), 0)
    for step in (4, 2, 1):
        keep = (sub & step) == 0
        out = []
        for k in range(step):
            a, b = value[:, k], value[:, k + step]
            rolled_a = pltpu.roll(a, 8 - step, 1)
            rolled_b = pltpu.roll(b, step, 1)
            out.append(jnp.where(keep, a, rolled_b) + jnp.where(keep, rolled_a, b))
        value = jnp.stack(out, axis=1)
    return value.reshape(groups * 8, 128)


NT = (((1,), (1,)), ((), ()))


def iota(shape, dim):
    return lax.broadcasted_iota(jnp.int32, shape, dim)


def fold_matrix():
    row, col = iota((128, 128), 0), iota((128, 128), 1)
    q = row >> 4
    number = jnp.where(q < 4, 2 * q, 2 * q - 7)
    re, im = wave(4 * number * ((col >> 1) & 7))
    from_im, to_im = (col & 1) == 1, ((row >> 3) & 1) == 1
    value = jnp.where(from_im == to_im, re, jnp.where(to_im, im, -im))
    return split(jnp.where((row & 7) == (col >> 4), value, 0.0))


def clifford_table():
    zeros = np.zeros((4, 4))
    first = (zeros, np.array([[0, 0, 0, 1], [0, 0, 1, 0], [0, -1, 0, 0], [-1, 0, 0, 0]]))
    second = (np.array([[0, 0, 0, -1], [0, 0, 1, 0], [0, 1, 0, 0], [-1, 0, 0, 0]]), zeros)
    third = (zeros, np.array([[0, 0, 1, 0], [0, 0, 0, -1], [-1, 0, 0, 0], [0, 1, 0, 0]]))
    fourth = (np.array([[0, 0, 1, 0], [0, 0, 0, 1], [1, 0, 0, 0], [0, 1, 0, 0]]), zeros)
    basis = [first, second, third, fourth]
    tables_re = []
    tables_im = []
    for mask in range(16):
        matrix_re = np.identity(4)
        matrix_im = np.zeros((4, 4))
        for bit in range(4):
            if mask >> bit & 1:
                basis_re, basis_im = basis[bit]
                new_re = matrix_re @ basis_re - matrix_im @ basis_im
                new_im = matrix_re @ basis_im + matrix_im @ basis_re
                matrix_re, matrix_im = (new_re, new_im)
        tables_re.append(matrix_re)
        tables_im.append(matrix_im)
    return (np.stack(tables_re), np.stack(tables_im))


def structures():
    table_re, table_im = clifford_table()
    out = []
    for re, im in zip(table_re, table_im, strict=True):
        matrix = im if im.any() else re
        columns = [int(np.flatnonzero(line)[0]) for line in matrix]
        signs = [float(line[k]) for line, k in zip(matrix, columns, strict=True)]
        out.append((bool(im.any()), columns, signs))
    return out


def write_vertices(spec, widen, slots, out_ref):
    keep = iota((8, 128), 1) < HALF
    lines = []
    for sink in range(12):
        half, k = divmod(sink, 6)
        for part in range(2):
            line = jnp.where(keep, spec[part, half], 0.0)
            lines.append(pltpu.roll(line, 128 - 12 * k, 1) if k else line)
    wide = jnp.concatenate(split(jnp.concatenate(lines, axis=0)), axis=1)
    wide = jnp.dot(wide, widen[...], preferred_element_type=F32)
    even = (iota((8, 384), 1) & 1) == 0
    left_re = [wide[16 * k : 16 * k + 8, :384] for k in range(12)]
    left_im = [wide[16 * k + 8 : 16 * k + 16, :384] for k in range(12)]
    right, turned = [], []
    for k in range(12):
        re, im = wide[16 * k : 16 * k + 8, 384:], wide[16 * k + 8 : 16 * k + 16, 384:]
        right.append(jnp.where(even, re, im))
        turned.append(jnp.where(even, im, -re))

    def pair(s, t):
        total = None
        for c in range(3):
            a, b = 3 * s + c, 3 * t + c
            term = left_re[a] * right[b] + left_im[a] * turned[b]
            total = term if total is None else total + term
        return total

    pairs = {}
    values = []
    for imaginary, columns, signs in structures():
        total = None
        for s in range(4):
            if (s, columns[s]) not in pairs:
                pairs[s, columns[s]] = pair(s, columns[s])
            term = pairs[s, columns[s]]
            if total is None:
                total = term if signs[s] > 0 else -term
            else:
                total = total + term if signs[s] > 0 else total - term
        if imaginary:
            total = jnp.where(even, -pltpu.roll(total, 383, 1), pltpu.roll(total, 1, 1))
        values.append(total)
    stacked = jnp.concatenate(split(jnp.concatenate(values, axis=0)), axis=0)
    out = lax.dot_general(
        stacked, slots[...], (((0,), (0,)), ((), ())), preferred_element_type=F32
    )
    for i in range(4):
        out_ref[i] = out[:288, i * 128 : i * 128 + 16]


def program_kernel(
    x_hbm, mom_smem, gamma_smem, out_ref,
    sbuf, gh, gl, w_high, w_low, x_wave, yall, pick, mom_all,
    before_buf, move_buf, widen, slots,
    zbuf, dbuf, hbuf, rbuf, spec,
    in_sems, mom_send, mom_recv, pair_send, pair_recv, far_send, far_recv, last_send, last_recv,
):
    gx, gz, ta = (lax.axis_index(name) for name in ("gx", "gz", "ta"))
    core, y_lo, z, y_hi = gz % 2, gz // 2, ta // 2, ta % 2
    y = y_hi * 2 + y_lo
    me = ((z * 4 + y) * 4 + gx) * 2 + core
    chip = (gx * 2 + y_lo) * 8 + ta
    xs = [gx] + [(gx + k) % 4 for k in range(1, 4)]
    ys = [y] + [(y + k) % 4 for k in range(1, 4)]
    zs = [z] + [(z + k) % 4 for k in range(1, 4)]
    cores = [core, 1 - core]
    gzs = [[(value % 2) * 2 + c for c in cores] for value in ys]
    tas = [[at_z * 2 + value // 2 for at_z in zs] for value in ys]
    hops = (0, 1, 2, 1)
    chips = sorted(
        ((dx, dy, dz) for dx in range(4) for dy in range(4) for dz in range(4)),
        key=lambda d: -sum(hops[k] for k in d),
    )

    def device(place, dc=0):
        dx, dy, dz = place
        return (xs[dx], gzs[dy][dc], tas[dy][dz])

    def chip_of(place):
        dx, dy, dz = place
        return (xs[dx] * 2 + ys[dy] % 2) * 8 + tas[dy][dz]

    barrier = pltpu.get_barrier_semaphore()
    stages = (
        [((dx, 0, 0), dc) for dx in (2, 1, 3, 0) for dc in (0, 1) if dx or dc],
        [((0, dy, 0), 0) for dy in (2, 1, 3)],
        [((0, 0, dz), 0) for dz in (2, 1, 3)],
    )
    for stage in stages:
        for place, dc in stage:
            pl.semaphore_signal(barrier, inc=1, device_id=device(place, dc), device_id_type=MESH)

    def load(k):
        part = pl.ds(k * 8, 8)
        return pltpu.make_async_copy(x_hbm.at[part], sbuf.at[part], in_sems.at[k])

    for k in range(CHUNKS):
        load(k).start()
    row = jnp.zeros((1, 128), jnp.int32)
    for i in range(4):
        for k in range(4):
            row = jnp.where(iota((1, 128), 1) == 4 * i + k, mom_smem[i, k], row)
    mom_all[me] = row

    fold_high, fold_low = fold_matrix()
    fold_twice = jnp.concatenate([fold_high, fold_high], axis=1)
    fold_rest = jnp.concatenate([fold_low, jnp.zeros_like(fold_low)], axis=1)[64:]

    def fold_step(k, carry):
        load(k).wait()
        for p in range(4):
            pair = k * 4 + p
            both = jnp.concatenate([sbuf[2 * pair], sbuf[2 * pair + 1]], axis=1)
            weights = jnp.concatenate(split(both), axis=0)
            out = jnp.dot(fold_twice, weights, preferred_element_type=F32)
            low = jnp.dot(fold_rest, weights, preferred_element_type=F32)
            out = jnp.concatenate([out[:64], out[64:] + low], axis=0)
            left = out[:, :128].reshape(16, 8, 128)
            right = out[:, 128:].reshape(16, 8, 128)
            high, rest = split(jnp.concatenate([left, right], axis=1))
            rows = pl.ds(pl.multiple_of(pair * 16, 16), 16)
            for q in range(8):
                for part in range(2):
                    lanes = slice(part * 128, part * 128 + 128)
                    gh[q, rows, lanes] = high[2 * q + part]
                    gl[q, rows, lanes] = rest[2 * q + part]
        return carry

    def spread(k):
        span = (1, 8, 32)[k]
        rows = mom_all.at[pl.ds(me // span * span, span)]
        for place, dc in stages[k]:
            pltpu.make_async_remote_copy(
                src_ref=rows, dst_ref=rows, send_sem=mom_send.at[k], recv_sem=mom_recv.at[k],
                device_id=device(place, dc), device_id_type=MESH,
            ).start()

    def moved(k):
        return mom_all.at[pl.ds(0, (7, 24, 96)[k])]

    def arrived(k):
        pltpu.make_async_copy(moved(k), moved(k), mom_recv.at[k]).wait()

    lax.fori_loop(0, 3, fold_step, 0)
    pl.semaphore_wait(barrier, 13)
    spread(0)
    lax.fori_loop(3, 11, fold_step, 0)
    arrived(0)
    spread(1)
    lax.fori_loop(11, CHUNKS, fold_step, 0)
    arrived(1)
    spread(2)

    before_buf[...] = (iota((512, 512), 0) < iota((512, 512), 1)).astype(F32).astype(BF16)
    to_row = iota((512, 512), 0)
    to_chip, to_core, own = to_row >> 3, (to_row >> 2) & 1, to_row & 3
    to_y = (to_chip & 1) * 2 + ((to_chip >> 3) & 1)
    source = own * 128 + ((to_chip >> 1) & 3) * 32 + to_y * 8 + (to_chip >> 4) * 2 + to_core
    move_buf[...] = (source == iota((512, 512), 1)).astype(F32).astype(BF16)
    lane = iota((128, 384), 1)
    source_a = (lane * 2731) >> 16
    source_b = (lane >> 1) - 12 * (((lane >> 1) * 5462) >> 16)
    for k, wanted in enumerate((source_a, source_b)):
        chosen = (iota((128, 384), 0) == wanted).astype(F32).astype(BF16)
        widen[:128, k * 384 : k * 384 + 384] = chosen
        widen[128:, k * 384 : k * 384 + 384] = chosen
    gamma_row = jnp.full((1, 128), -1, jnp.int32)
    for k in range(16):
        gamma_row = jnp.where(iota((1, 128), 1) == k, gamma_smem[k], gamma_row)
    row = iota((128, 128), 0)
    for i in range(4):
        chosen = ((row >> 3) == gamma_row) & ((row & 7) == core * 4 + i)
        chosen = chosen.astype(F32).astype(BF16)
        slots[:128, i * 128 : i * 128 + 128] = chosen
        slots[128:, i * 128 : i * 128 + 128] = chosen
    arrived(2)

    turned = jnp.transpose((mom_all[...].reshape(128, 128) & 31).astype(F32))
    mom = jnp.concatenate([turned[4 * i : 4 * i + 4] for i in range(4)], axis=1)
    ny = mom[1:2].astype(jnp.int32)
    cls = ((ny >> 1) & 3) + 4 * (ny & 1)
    member = (iota((8, 512), 0) == cls).astype(F32)
    ahead = jnp.dot(member.astype(BF16), before_buf[...], preferred_element_type=F32)
    slot = jnp.sum(member * ahead, axis=0, keepdims=True)
    ends = []
    start = jnp.int32(0)
    for q in range(8):
        count = jnp.sum(member[q : q + 1]).astype(jnp.int32)
        slot = slot + member[q : q + 1] * (start * 128).astype(F32)
        start = start + ((count + 127) >> 7)
        ends.append(start)
    slot = slot.astype(jnp.int32)
    mom8 = jnp.concatenate([mom, jnp.zeros_like(mom)], axis=0).astype(BF16)
    digits = jnp.concatenate([slot >> 5, slot & 31] + [slot * 0] * 6, axis=0).astype(F32).astype(BF16)
    column = lax.dot_general(move_buf[...], digits, NT, preferred_element_type=F32)
    column = (column[:, 0:1] * 32.0 + column[:, 1:2]).astype(jnp.int32)

    def prepare(j):
        here = (iota((128, 512), 0) + j * 128 == slot).astype(F32).astype(BF16)
        sorted_mom = lax.dot_general(mom8, here, NT, preferred_element_type=F32).astype(jnp.int32)
        nx, ny, nz, nt = (sorted_mom[i : i + 1] for i in range(4))
        site = iota((32, 128), 0)
        zr, zi = wave(nz * (site >> 2) + nt * (site & 3))
        yr, yi = wave(ny * iota((8, 128), 0))
        pr = jnp.concatenate([zr * yr[k : k + 1] - zi * yi[k : k + 1] for k in range(4)], 0)
        pi = jnp.concatenate([zr * yi[k : k + 1] + zi * yr[k : k + 1] for k in range(4)], 0)
        (prh, prl), (pih, pil) = split(pr), split(pi)
        w_high[j] = jnp.concatenate(
            [jnp.concatenate([prh, pih], 1), jnp.concatenate([-pih, prh], 1)], 0
        )
        w_low[j] = jnp.concatenate(
            [jnp.concatenate([prl, pil], 1), jnp.concatenate([-pil, prl], 1)], 0
        )
        xr, xi = wave(nx * (gx * 8 + iota((8, 128), 0)) + nz * (gz * 8) + nt * (ta * 4))
        x_wave[j, 0] = xr
        x_wave[j, 1] = xi

    def multiply(j, half):
        q = jnp.int32(0)
        for end in ends[:7]:
            q = q + (end <= j).astype(jnp.int32)
        rows = pl.ds(half * HALF * 8, HALF * 8)
        high = gh[q, rows]
        top = w_high[j]
        out = (
            jnp.dot(high, top, preferred_element_type=F32)
            + jnp.dot(gl[q, rows], top, preferred_element_type=F32)
            + jnp.dot(high, w_low[j], preferred_element_type=F32)
        )
        xr, xi = x_wave[j, 0], x_wave[j, 1]
        re = out[:, :128].reshape(HALF, 8, 128)
        im = out[:, 128:].reshape(HALF, 8, 128)
        lanes = pl.ds(pl.multiple_of(j * 256, 256), 128)
        lanes_low = pl.ds(pl.multiple_of(j * 256 + 128, 128), 128)
        for part, value in enumerate((re * xr - im * xi, re * xi + im * xr)):
            first, rest = split(sum_over_x(value))
            to = pl.ds(part * 128, HALF)
            yall[half, to, lanes] = first
            yall[half, to, lanes_low] = rest

    def choose(j):
        lanes = pl.ds(pl.multiple_of(j * 256, 256), 128)
        lanes_low = pl.ds(pl.multiple_of(j * 256 + 128, 128), 128)
        chosen = (iota((512, 128), 1) + j * 128 == column).astype(F32).astype(BF16)
        pick[:, lanes] = chosen
        pick[:, lanes_low] = chosen

    def first_step(j, carry):
        multiply(j, 0)
        prepare(j + 1)
        choose(j)
        return carry

    def second_step(j, carry):
        multiply(j, 1)
        return carry

    def to_partner(half):
        return pltpu.make_async_remote_copy(
            src_ref=zbuf.at[half, 1 - core], dst_ref=dbuf.at[half],
            send_sem=pair_send.at[half], recv_sem=pair_recv.at[half],
            device_id=device((0, 0, 0), 1), device_id_type=MESH,
        )

    def restore(half):
        back = lax.dot_general(pick[...], yall[half], NT, preferred_element_type=F32)
        zbuf[half, 0] = back[:, :128]
        zbuf[half, 1] = back[:, 128:]
        to_partner(half).start()

    def send_far(half):
        to_partner(half).wait_recv()
        total = (zbuf[half, core] + dbuf[half]) * (1.0 / math.sqrt(float(LX * LY * LZ * LT)))
        hbuf[half] = total.reshape(64, 8, 128)
        rbuf[half, chip] = hbuf[half, chip]
        for place in chips[:-1]:
            pltpu.make_async_remote_copy(
                src_ref=hbuf.at[half, chip_of(place)], dst_ref=rbuf.at[half, chip],
                send_sem=far_send.at[half], recv_sem=far_recv.at[half],
                device_id=device(place), device_id_type=MESH,
            ).start()

    def wait_far(half):
        blocks = rbuf.at[half, pl.ds(0, 63)]
        pltpu.make_async_copy(blocks, blocks, far_recv.at[half]).wait()
        spec[core, half] = jnp.sum(rbuf[half], axis=0)

    prepare(jnp.int32(0))
    lax.fori_loop(0, TILES, first_step, 0)
    restore(0)
    lax.fori_loop(0, TILES // 2, second_step, 0)
    send_far(0)
    lax.fori_loop(TILES // 2, TILES, second_step, 0)
    restore(1)
    send_far(1)
    wait_far(0)
    wait_far(1)
    last = pltpu.make_async_remote_copy(
        src_ref=spec.at[core], dst_ref=spec.at[core], send_sem=last_send, recv_sem=last_recv,
        device_id=device((0, 0, 0), 1), device_id_type=MESH,
    )
    last.start()
    for k in range(3):
        pltpu.make_async_copy(moved(k), moved(k), mom_send.at[k]).wait()
    for half in range(2):
        to_partner(half).wait_send()
        blocks = hbuf.at[half, pl.ds(0, 63)]
        pltpu.make_async_copy(blocks, blocks, far_send.at[half]).wait()
    last.wait()
    write_vertices(spec, widen, slots, out_ref)


def vertices_kernel_call(x, momenta, gamma_index):
    vmem = pl.BlockSpec(memory_space=pltpu.VMEM)
    dma = pltpu.SemaphoreType.DMA
    return pl.pallas_call(
        program_kernel,
        out_shape=jax.ShapeDtypeStruct((4, 288, 16), F32),
        in_specs=[pl.BlockSpec(memory_space=pl.ANY)]
        + [pl.BlockSpec(memory_space=pltpu.SMEM)] * 2,
        out_specs=vmem,
        scratch_shapes=[
            pltpu.VMEM((144, 128, 128), F32),
            pltpu.VMEM((8, 1152, 256), BF16),
            pltpu.VMEM((8, 1152, 256), BF16),
            pltpu.VMEM((TILES + 1, 256, 256), BF16),
            pltpu.VMEM((TILES + 1, 256, 256), BF16),
            pltpu.VMEM((TILES + 1, 2, 8, 128), F32),
            pltpu.VMEM((2, 256, TILES * 256), BF16),
            pltpu.VMEM((512, TILES * 256), BF16),
            pltpu.VMEM((128, 1, 128), jnp.int32),
            pltpu.VMEM((512, 512), BF16),
            pltpu.VMEM((512, 512), BF16),
            pltpu.VMEM((256, 768), BF16),
            pltpu.VMEM((256, 512), BF16),
            pltpu.VMEM((2, 2, 512, 128), F32),
            pltpu.VMEM((2, 512, 128), F32),
            pltpu.VMEM((2, 64, 8, 128), F32),
            pltpu.VMEM((2, 64, 8, 128), F32),
            pltpu.VMEM((2, 2, 8, 128), F32),
            dma((CHUNKS,)),
            dma((3,)), dma((3,)), dma((2,)), dma((2,)), dma((2,)), dma((2,)), dma, dma,
        ],
        compiler_params=pltpu.CompilerParams(
            collective_id=0, has_side_effects=True, vmem_limit_bytes=56 * 1024 * 1024
        ),
    )(x, momenta, gamma_index)


def site_major(propagator):
    x = jnp.transpose(propagator, (1, 2, 0, 3)).reshape(144, 2, 64, 128)
    return jnp.transpose(x, (0, 2, 1, 3)).reshape(144, 128, 128)


def body(propagator, momenta, gamma_index):
    out = vertices_kernel_call(site_major(propagator), momenta, gamma_index)
    return jnp.transpose(out.reshape(4, 12, 12, 2, 16), (0, 4, 3, 1, 2))


def solution(mesh):
    placed = (P(None, None, None, ("gx", "gz", "ta")), P(("gx", "gz", "ta"), None), P())
    return jax.shard_map(
        body,
        mesh=mesh,
        in_specs=placed,
        out_specs=P(("gx", "gz", "ta"), None, None, None, None),
        check_vma=False,
    )
```

```python
import math

import jax
import jax.numpy as jnp
import numpy as np
from jax import lax
from jax.experimental import pallas as pl
from jax.experimental.pallas import tpu as pltpu
from jax.sharding import PartitionSpec as P

LX = LY = LZ = LT = 32
MESH = pl.DeviceIdType.MESH
F32 = jnp.float32
BF16 = jnp.bfloat16
TILES = 11
CHUNKS = 18
HALF = 72


def split(value):
    high = value.astype(BF16)
    return high, (value - high.astype(F32)).astype(BF16)


def sine(index):
    turn = ((index + 16) & 31) - 16
    turn = jnp.where(turn > 8, 16 - turn, jnp.where(turn < -8, -16 - turn, turn))
    u = turn.astype(F32) * (math.pi / 16)
    s = u * u
    poly = 1 / 362880 - s * (1 / 39916800)
    for factor in (-1 / 5040, 1 / 120, -1 / 6, 1.0):
        poly = factor + s * poly
    return u * poly


def wave(index):
    return sine(index + 8), -sine(index)


def sum_over_x(value):
    groups = value.shape[0] // 8
    value = value.reshape(groups, 8, 8, 128)
    sub = lax.broadcasted_iota(jnp.int32, (8, 128), 0)
    for step in (4, 2, 1):
        keep = (sub & step) == 0
        out = []
        for k in range(step):
            a, b = value[:, k], value[:, k + step]
            rolled_a = pltpu.roll(a, 8 - step, 1)
            rolled_b = pltpu.roll(b, step, 1)
            out.append(jnp.where(keep, a, rolled_b) + jnp.where(keep, rolled_a, b))
        value = jnp.stack(out, axis=1)
    return value.reshape(groups * 8, 128)


NT = (((1,), (1,)), ((), ()))


def iota(shape, dim):
    return lax.broadcasted_iota(jnp.int32, shape, dim)


def fold_matrix():
    row, col = iota((128, 128), 0), iota((128, 128), 1)
    q = row >> 4
    number = jnp.where(q < 4, 2 * q, 2 * q - 7)
    re, im = wave(4 * number * ((col >> 1) & 7))
    from_im, to_im = (col & 1) == 1, ((row >> 3) & 1) == 1
    value = jnp.where(from_im == to_im, re, jnp.where(to_im, im, -im))
    return split(jnp.where((row & 7) == (col >> 4), value, 0.0))


def clifford_table():
    zeros = np.zeros((4, 4))
    first = (zeros, np.array([[0, 0, 0, 1], [0, 0, 1, 0], [0, -1, 0, 0], [-1, 0, 0, 0]]))
    second = (np.array([[0, 0, 0, -1], [0, 0, 1, 0], [0, 1, 0, 0], [-1, 0, 0, 0]]), zeros)
    third = (zeros, np.array([[0, 0, 1, 0], [0, 0, 0, -1], [-1, 0, 0, 0], [0, 1, 0, 0]]))
    fourth = (np.array([[0, 0, 1, 0], [0, 0, 0, 1], [1, 0, 0, 0], [0, 1, 0, 0]]), zeros)
    basis = [first, second, third, fourth]
    tables_re = []
    tables_im = []
    for mask in range(16):
        matrix_re = np.identity(4)
        matrix_im = np.zeros((4, 4))
        for bit in range(4):
            if mask >> bit & 1:
                basis_re, basis_im = basis[bit]
                new_re = matrix_re @ basis_re - matrix_im @ basis_im
                new_im = matrix_re @ basis_im + matrix_im @ basis_re
                matrix_re, matrix_im = (new_re, new_im)
        tables_re.append(matrix_re)
        tables_im.append(matrix_im)
    return (np.stack(tables_re), np.stack(tables_im))


def structures():
    table_re, table_im = clifford_table()
    out = []
    for re, im in zip(table_re, table_im, strict=True):
        matrix = im if im.any() else re
        columns = [int(np.flatnonzero(line)[0]) for line in matrix]
        signs = [float(line[k]) for line, k in zip(matrix, columns, strict=True)]
        out.append((bool(im.any()), columns, signs))
    return out


def write_vertices(spec, widen, slots, out_ref):
    keep = iota((8, 128), 1) < HALF
    lines = []
    for sink in range(12):
        half, k = divmod(sink, 6)
        for part in range(2):
            line = jnp.where(keep, spec[part, half], 0.0)
            lines.append(pltpu.roll(line, 128 - 12 * k, 1) if k else line)
    wide = jnp.concatenate(split(jnp.concatenate(lines, axis=0)), axis=1)
    wide = jnp.dot(wide, widen[...], preferred_element_type=F32)
    even = (iota((8, 384), 1) & 1) == 0
    left_re = [wide[16 * k : 16 * k + 8, :384] for k in range(12)]
    left_im = [wide[16 * k + 8 : 16 * k + 16, :384] for k in range(12)]
    right, turned = [], []
    for k in range(12):
        re, im = wide[16 * k : 16 * k + 8, 384:], wide[16 * k + 8 : 16 * k + 16, 384:]
        right.append(jnp.where(even, re, im))
        turned.append(jnp.where(even, im, -re))

    def pair(s, t):
        total = None
        for c in range(3):
            a, b = 3 * s + c, 3 * t + c
            term = left_re[a] * right[b] + left_im[a] * turned[b]
            total = term if total is None else total + term
        return total

    pairs = {}
    values = []
    for imaginary, columns, signs in structures():
        total = None
        for s in range(4):
            if (s, columns[s]) not in pairs:
                pairs[s, columns[s]] = pair(s, columns[s])
            term = pairs[s, columns[s]]
            if total is None:
                total = term if signs[s] > 0 else -term
            else:
                total = total + term if signs[s] > 0 else total - term
        if imaginary:
            total = jnp.where(even, -pltpu.roll(total, 383, 1), pltpu.roll(total, 1, 1))
        values.append(total)
    stacked = jnp.concatenate(split(jnp.concatenate(values, axis=0)), axis=0)
    out = lax.dot_general(
        stacked, slots[...], (((0,), (0,)), ((), ())), preferred_element_type=F32
    )
    for i in range(4):
        out_ref[i] = out[:288, i * 128 : i * 128 + 16]


def program_kernel(
    x_hbm, mom_smem, gamma_smem, out_ref,
    sbuf, gh, gl, w_high, w_low, x_wave, raw_even, raw_odd, yall, pick, mom_all,
    before_buf, move_buf, widen, slots,
    zbuf, dbuf, hbuf, rbuf, spec,
    in_sems, mom_send, mom_recv, pair_send, pair_recv, far_send, far_recv, last_send, last_recv,
):
    gx, gz, ta = (lax.axis_index(name) for name in ("gx", "gz", "ta"))
    core, y_lo, z, y_hi = gz % 2, gz // 2, ta // 2, ta % 2
    y = y_hi * 2 + y_lo
    me = ((z * 4 + y) * 4 + gx) * 2 + core
    chip = (gx * 2 + y_lo) * 8 + ta
    xs = [gx] + [(gx + k) % 4 for k in range(1, 4)]
    ys = [y] + [(y + k) % 4 for k in range(1, 4)]
    zs = [z] + [(z + k) % 4 for k in range(1, 4)]
    cores = [core, 1 - core]
    gzs = [[(value % 2) * 2 + c for c in cores] for value in ys]
    tas = [[at_z * 2 + value // 2 for at_z in zs] for value in ys]
    hops = (0, 1, 2, 1)
    chips = sorted(
        ((dx, dy, dz) for dx in range(4) for dy in range(4) for dz in range(4)),
        key=lambda d: -sum(hops[k] for k in d),
    )

    def device(place, dc=0):
        dx, dy, dz = place
        return (xs[dx], gzs[dy][dc], tas[dy][dz])

    def chip_of(place):
        dx, dy, dz = place
        return (xs[dx] * 2 + ys[dy] % 2) * 8 + tas[dy][dz]

    barrier = pltpu.get_barrier_semaphore()
    others = [(place, dc) for place in chips for dc in (0, 1) if place != (0, 0, 0) or dc]
    for place, dc in others:
        pl.semaphore_signal(barrier, inc=1, device_id=device(place, dc), device_id_type=MESH)

    def load(k):
        part = pl.ds(k * 8, 8)
        return pltpu.make_async_copy(x_hbm.at[part], sbuf.at[part], in_sems.at[k])

    for k in range(CHUNKS):
        load(k).start()
    row = jnp.zeros((1, 128), jnp.int32)
    for i in range(4):
        for k in range(4):
            row = jnp.where(iota((1, 128), 1) == 4 * i + k, mom_smem[i, k], row)
    mom_all[me] = row

    fold_high, fold_low = fold_matrix()
    fold_twice = jnp.concatenate([fold_high, fold_high], axis=1)
    fold_rest = jnp.concatenate([fold_low, jnp.zeros_like(fold_low)], axis=1)[64:]

    def fold_step(k, carry):
        load(k).wait()
        for p in range(4):
            pair = k * 4 + p
            both = jnp.concatenate([sbuf[2 * pair], sbuf[2 * pair + 1]], axis=1)
            weights = jnp.concatenate(split(both), axis=0)
            out = jnp.dot(fold_twice, weights, preferred_element_type=F32)
            low = jnp.dot(fold_rest, weights, preferred_element_type=F32)
            out = jnp.concatenate([out[:64], out[64:] + low], axis=0)
            left = out[:, :128].reshape(16, 8, 128)
            right = out[:, 128:].reshape(16, 8, 128)
            high, rest = split(jnp.concatenate([left, right], axis=1))
            rows = pl.ds(pl.multiple_of(pair * 16, 16), 16)
            for q in range(8):
                for part in range(2):
                    lanes = slice(part * 128, part * 128 + 128)
                    gh[q, rows, lanes] = high[2 * q + part]
                    gl[q, rows, lanes] = rest[2 * q + part]
        return carry

    lax.fori_loop(0, 10, fold_step, 0)
    pl.semaphore_wait(barrier, 127)
    for place, dc in others:
        pltpu.make_async_remote_copy(
            src_ref=mom_all.at[me], dst_ref=mom_all.at[me], send_sem=mom_send, recv_sem=mom_recv,
            device_id=device(place, dc), device_id_type=MESH,
        ).start()
    lax.fori_loop(10, CHUNKS, fold_step, 0)

    before_buf[...] = (iota((512, 512), 0) < iota((512, 512), 1)).astype(F32).astype(BF16)
    to_row = iota((512, 512), 1)
    to_chip, to_core, own = to_row >> 3, (to_row >> 2) & 1, to_row & 3
    to_y = (to_chip & 1) * 2 + ((to_chip >> 3) & 1)
    source = own * 128 + ((to_chip >> 1) & 3) * 32 + to_y * 8 + (to_chip >> 4) * 2 + to_core
    move_buf[...] = (source == iota((512, 512), 0)).astype(F32).astype(BF16)
    lane = iota((128, 384), 1)
    source_a = (lane * 2731) >> 16
    source_b = (lane >> 1) - 12 * (((lane >> 1) * 5462) >> 16)
    for k, wanted in enumerate((source_a, source_b)):
        chosen = (iota((128, 384), 0) == wanted).astype(F32).astype(BF16)
        widen[:128, k * 384 : k * 384 + 384] = chosen
        widen[128:, k * 384 : k * 384 + 384] = chosen
    gamma_row = jnp.full((1, 128), -1, jnp.int32)
    for k in range(16):
        gamma_row = jnp.where(iota((1, 128), 1) == k, gamma_smem[k], gamma_row)
    row = iota((128, 128), 0)
    for i in range(4):
        chosen = ((row >> 3) == gamma_row) & ((row & 7) == core * 4 + i)
        chosen = chosen.astype(F32).astype(BF16)
        slots[:128, i * 128 : i * 128 + 128] = chosen
        slots[128:, i * 128 : i * 128 + 128] = chosen
    all_rows = mom_all.at[pl.ds(0, 127)]
    pltpu.make_async_copy(all_rows, all_rows, mom_recv).wait()

    turned = jnp.transpose((mom_all[...].reshape(128, 128) & 31).astype(F32))
    mom = jnp.concatenate([turned[4 * i : 4 * i + 4] for i in range(4)], axis=1)
    mom8 = jnp.concatenate([mom, jnp.zeros_like(mom)], axis=0).astype(BF16)
    mom8 = jnp.dot(mom8, move_buf[...], preferred_element_type=F32)
    ny = mom8[1:2].astype(jnp.int32)
    mom8 = mom8.astype(BF16)
    cls = ((ny >> 1) & 3) + 4 * (ny & 1)
    member = (iota((8, 512), 0) == cls).astype(F32)
    ahead = jnp.dot(member.astype(BF16), before_buf[...], preferred_element_type=F32)
    slot = jnp.sum(member * ahead, axis=0, keepdims=True)
    ends = []
    start = jnp.int32(0)
    for q in range(8):
        count = jnp.sum(member[q : q + 1]).astype(jnp.int32)
        slot = slot + member[q : q + 1] * (start * 128).astype(F32)
        start = start + ((count + 127) >> 7)
        ends.append(start)
    slot = slot.astype(jnp.int32)
    def prepare(j):
        here = (iota((128, 512), 0) + j * 128 == slot).astype(F32).astype(BF16)
        pick[pl.ds(pl.multiple_of(j * 128, 128), 128)] = here
        sorted_mom = lax.dot_general(mom8, here, NT, preferred_element_type=F32).astype(jnp.int32)
        nx, ny, nz, nt = (sorted_mom[i : i + 1] for i in range(4))
        site = iota((32, 128), 0)
        zr, zi = wave(nz * (site >> 2) + nt * (site & 3))
        yr, yi = wave(ny * iota((8, 128), 0))
        pr = jnp.concatenate([zr * yr[k : k + 1] - zi * yi[k : k + 1] for k in range(4)], 0)
        pi = jnp.concatenate([zr * yi[k : k + 1] + zi * yr[k : k + 1] for k in range(4)], 0)
        (prh, prl), (pih, pil) = split(pr), split(pi)
        w_high[j] = jnp.concatenate(
            [jnp.concatenate([prh, pih], 1), jnp.concatenate([-pih, prh], 1)], 0
        )
        w_low[j] = jnp.concatenate(
            [jnp.concatenate([prl, pil], 1), jnp.concatenate([-pil, prl], 1)], 0
        )
        xr, xi = wave(nx * (gx * 8 + iota((8, 128), 0)) + nz * (gz * 8) + nt * (ta * 4))
        x_wave[j, 0] = xr
        x_wave[j, 1] = xi

    def multiply(j, half):
        q = jnp.int32(0)
        for end in ends[:7]:
            q = q + (end <= j).astype(jnp.int32)
        rows = pl.ds(half * HALF * 8, HALF * 8)
        high = gh[q, rows]
        top = w_high[j]
        return (
            jnp.dot(high, top, preferred_element_type=F32)
            + jnp.dot(gl[q, rows], top, preferred_element_type=F32)
            + jnp.dot(high, w_low[j], preferred_element_type=F32)
        )

    def finish(raw, j, half):
        xr, xi = x_wave[j, 0], x_wave[j, 1]
        re = raw[:, :128].reshape(HALF, 8, 128)
        im = raw[:, 128:].reshape(HALF, 8, 128)
        lanes = pl.ds(pl.multiple_of(j * 128, 128), 128)
        for part, value in enumerate((re * xr - im * xi, re * xi + im * xr)):
            first, rest = split(sum_over_x(value))
            yall[half, pl.ds(part * HALF, HALF), lanes] = first
            yall[half, pl.ds((2 + part) * HALF, HALF), lanes] = rest

    def two_tiles(half):
        def step(i, carry):
            out = multiply(2 * i, half)
            finish(raw_odd, (2 * i + TILES) % (TILES + 1), half)
            if half == 0:
                prepare(2 * i + 2)
            raw_even[...] = out
            out = multiply(2 * i + 1, half)
            finish(raw_even, 2 * i, half)
            if half == 0:
                prepare(2 * i + 3)
            raw_odd[...] = out
            return carry

        return step

    def to_partner(half):
        return pltpu.make_async_remote_copy(
            src_ref=zbuf.at[half, 1 - core], dst_ref=dbuf.at[half],
            send_sem=pair_send.at[half], recv_sem=pair_recv.at[half],
            device_id=device((0, 0, 0), 1), device_id_type=MESH,
        )

    def restore(half):
        back = jnp.dot(
            yall[half, :, : TILES * 128], pick[: TILES * 128], preferred_element_type=F32
        )
        back = back[: 2 * HALF] + back[2 * HALF :]
        fill = jnp.zeros((128 - HALF, 512), F32)
        for part in range(2):
            rows = jnp.concatenate([back[part * HALF : (part + 1) * HALF], fill], axis=0)
            zbuf[half, part] = jnp.transpose(rows)
        to_partner(half).start()

    def send_far(half):
        to_partner(half).wait_recv()
        total = (zbuf[half, core] + dbuf[half]) * (1.0 / math.sqrt(float(LX * LY * LZ * LT)))
        hbuf[half] = total.reshape(64, 8, 128)
        rbuf[half, chip] = hbuf[half, chip]
        for place in chips[:-1]:
            pltpu.make_async_remote_copy(
                src_ref=hbuf.at[half, chip_of(place)], dst_ref=rbuf.at[half, chip],
                send_sem=far_send.at[half], recv_sem=far_recv.at[half],
                device_id=device(place), device_id_type=MESH,
            ).start()

    def wait_far(half):
        blocks = rbuf.at[half, pl.ds(0, 63)]
        pltpu.make_async_copy(blocks, blocks, far_recv.at[half]).wait()
        spec[core, half] = jnp.sum(rbuf[half], axis=0)

    prepare(jnp.int32(0))
    prepare(jnp.int32(1))
    steps = (TILES + 1) // 2
    lax.fori_loop(0, steps, two_tiles(0), 0)
    restore(0)
    lax.fori_loop(0, steps // 2, two_tiles(1), 0)
    send_far(0)
    lax.fori_loop(steps // 2, steps, two_tiles(1), 0)
    restore(1)
    send_far(1)
    wait_far(0)
    wait_far(1)
    last = pltpu.make_async_remote_copy(
        src_ref=spec.at[core], dst_ref=spec.at[core], send_sem=last_send, recv_sem=last_recv,
        device_id=device((0, 0, 0), 1), device_id_type=MESH,
    )
    last.start()
    pltpu.make_async_copy(all_rows, all_rows, mom_send).wait()
    for half in range(2):
        to_partner(half).wait_send()
        blocks = hbuf.at[half, pl.ds(0, 63)]
        pltpu.make_async_copy(blocks, blocks, far_send.at[half]).wait()
    last.wait()
    write_vertices(spec, widen, slots, out_ref)


def vertices_kernel_call(x, momenta, gamma_index):
    vmem = pl.BlockSpec(memory_space=pltpu.VMEM)
    dma = pltpu.SemaphoreType.DMA
    return pl.pallas_call(
        program_kernel,
        out_shape=jax.ShapeDtypeStruct((4, 288, 16), F32),
        in_specs=[pl.BlockSpec(memory_space=pl.ANY)]
        + [pl.BlockSpec(memory_space=pltpu.SMEM)] * 2,
        out_specs=vmem,
        scratch_shapes=[
            pltpu.VMEM((144, 128, 128), F32),
            pltpu.VMEM((8, 1152, 256), BF16),
            pltpu.VMEM((8, 1152, 256), BF16),
            pltpu.VMEM((TILES + 3, 256, 256), BF16),
            pltpu.VMEM((TILES + 3, 256, 256), BF16),
            pltpu.VMEM((TILES + 3, 2, 8, 128), F32),
            pltpu.VMEM((HALF * 8, 256), F32),
            pltpu.VMEM((HALF * 8, 256), F32),
            pltpu.VMEM((2, 4 * HALF, (TILES + 1) * 128), BF16),
            pltpu.VMEM(((TILES + 3) * 128, 512), BF16),
            pltpu.VMEM((128, 1, 128), jnp.int32),
            pltpu.VMEM((512, 512), BF16),
            pltpu.VMEM((512, 512), BF16),
            pltpu.VMEM((256, 768), BF16),
            pltpu.VMEM((256, 512), BF16),
            pltpu.VMEM((2, 2, 512, 128), F32),
            pltpu.VMEM((2, 512, 128), F32),
            pltpu.VMEM((2, 64, 8, 128), F32),
            pltpu.VMEM((2, 64, 8, 128), F32),
            pltpu.VMEM((2, 2, 8, 128), F32),
            dma((CHUNKS,)),
            dma, dma, dma((2,)), dma((2,)), dma((2,)), dma((2,)), dma, dma,
        ],
        compiler_params=pltpu.CompilerParams(
            collective_id=0, has_side_effects=True, vmem_limit_bytes=56 * 1024 * 1024
        ),
    )(x, momenta, gamma_index)


def site_major(propagator):
    x = jnp.transpose(propagator, (1, 2, 0, 3)).reshape(144, 2, 64, 128)
    return jnp.transpose(x, (0, 2, 1, 3)).reshape(144, 128, 128)


def body(propagator, momenta, gamma_index):
    out = vertices_kernel_call(site_major(propagator), momenta, gamma_index)
    return jnp.transpose(out.reshape(4, 12, 12, 2, 16), (0, 4, 3, 1, 2))


def solution(mesh):
    placed = (P(None, None, None, ("gx", "gz", "ta")), P(("gx", "gz", "ta"), None), P())
    return jax.shard_map(
        body,
        mesh=mesh,
        in_specs=placed,
        out_specs=P(("gx", "gz", "ta"), None, None, None, None),
        check_vma=False,
    )
```

```python
import math

import jax
import jax.numpy as jnp
import numpy as np
from jax import lax
from jax.experimental import pallas as pl
from jax.experimental.pallas import tpu as pltpu
from jax.sharding import PartitionSpec as P

LX = LY = LZ = LT = 32
MESH = pl.DeviceIdType.MESH
F32 = jnp.float32
BF16 = jnp.bfloat16
TILES = 11
CHUNKS = 18
HALF = 72


def split(value):
    high = value.astype(BF16)
    return high, (value - high.astype(F32)).astype(BF16)


def sine(index):
    turn = ((index + 16) & 31) - 16
    turn = jnp.where(turn > 8, 16 - turn, jnp.where(turn < -8, -16 - turn, turn))
    u = turn.astype(F32) * (math.pi / 16)
    s = u * u
    poly = 1 / 362880 - s * (1 / 39916800)
    for factor in (-1 / 5040, 1 / 120, -1 / 6, 1.0):
        poly = factor + s * poly
    return u * poly


def wave(index):
    return sine(index + 8), -sine(index)


def sum_over_x(value):
    groups = value.shape[0] // 8
    value = value.reshape(groups, 8, 8, 128)
    sub = lax.broadcasted_iota(jnp.int32, (8, 128), 0)
    for step in (4, 2, 1):
        keep = (sub & step) == 0
        out = []
        for k in range(step):
            a, b = value[:, k], value[:, k + step]
            rolled_a = pltpu.roll(a, 8 - step, 1)
            rolled_b = pltpu.roll(b, step, 1)
            out.append(jnp.where(keep, a, rolled_b) + jnp.where(keep, rolled_a, b))
        value = jnp.stack(out, axis=1)
    return value.reshape(groups * 8, 128)


NT = (((1,), (1,)), ((), ()))


def iota(shape, dim):
    return lax.broadcasted_iota(jnp.int32, shape, dim)


def fold_matrix():
    row, col = iota((128, 128), 0), iota((128, 128), 1)
    q = row >> 4
    number = jnp.where(q < 4, 2 * q, 2 * q - 7)
    re, im = wave(4 * number * ((col >> 1) & 7))
    from_im, to_im = (col & 1) == 1, ((row >> 3) & 1) == 1
    value = jnp.where(from_im == to_im, re, jnp.where(to_im, im, -im))
    return split(jnp.where((row & 7) == (col >> 4), value, 0.0))


def clifford_table():
    zeros = np.zeros((4, 4))
    first = (zeros, np.array([[0, 0, 0, 1], [0, 0, 1, 0], [0, -1, 0, 0], [-1, 0, 0, 0]]))
    second = (np.array([[0, 0, 0, -1], [0, 0, 1, 0], [0, 1, 0, 0], [-1, 0, 0, 0]]), zeros)
    third = (zeros, np.array([[0, 0, 1, 0], [0, 0, 0, -1], [-1, 0, 0, 0], [0, 1, 0, 0]]))
    fourth = (np.array([[0, 0, 1, 0], [0, 0, 0, 1], [1, 0, 0, 0], [0, 1, 0, 0]]), zeros)
    basis = [first, second, third, fourth]
    tables_re = []
    tables_im = []
    for mask in range(16):
        matrix_re = np.identity(4)
        matrix_im = np.zeros((4, 4))
        for bit in range(4):
            if mask >> bit & 1:
                basis_re, basis_im = basis[bit]
                new_re = matrix_re @ basis_re - matrix_im @ basis_im
                new_im = matrix_re @ basis_im + matrix_im @ basis_re
                matrix_re, matrix_im = (new_re, new_im)
        tables_re.append(matrix_re)
        tables_im.append(matrix_im)
    return (np.stack(tables_re), np.stack(tables_im))


def structures():
    table_re, table_im = clifford_table()
    out = []
    for re, im in zip(table_re, table_im, strict=True):
        matrix = im if im.any() else re
        columns = [int(np.flatnonzero(line)[0]) for line in matrix]
        signs = [float(line[k]) for line, k in zip(matrix, columns, strict=True)]
        out.append((bool(im.any()), columns, signs))
    return out


def write_vertices(spec, widen, slots, out_ref):
    keep = iota((8, 128), 1) < HALF
    lines = []
    for sink in range(12):
        half, k = divmod(sink, 6)
        for part in range(2):
            line = jnp.where(keep, spec[part, half], 0.0)
            lines.append(pltpu.roll(line, 128 - 12 * k, 1) if k else line)
    wide = jnp.concatenate(split(jnp.concatenate(lines, axis=0)), axis=1)
    wide = jnp.dot(wide, widen[...], preferred_element_type=F32)
    even = (iota((8, 384), 1) & 1) == 0
    left_re = [wide[16 * k : 16 * k + 8, :384] for k in range(12)]
    left_im = [wide[16 * k + 8 : 16 * k + 16, :384] for k in range(12)]
    right, turned = [], []
    for k in range(12):
        re, im = wide[16 * k : 16 * k + 8, 384:], wide[16 * k + 8 : 16 * k + 16, 384:]
        right.append(jnp.where(even, re, im))
        turned.append(jnp.where(even, im, -re))

    def pair(s, t):
        total = None
        for c in range(3):
            a, b = 3 * s + c, 3 * t + c
            term = left_re[a] * right[b] + left_im[a] * turned[b]
            total = term if total is None else total + term
        return total

    pairs = {}
    values = []
    for imaginary, columns, signs in structures():
        total = None
        for s in range(4):
            if (s, columns[s]) not in pairs:
                pairs[s, columns[s]] = pair(s, columns[s])
            term = pairs[s, columns[s]]
            if total is None:
                total = term if signs[s] > 0 else -term
            else:
                total = total + term if signs[s] > 0 else total - term
        if imaginary:
            total = jnp.where(even, -pltpu.roll(total, 383, 1), pltpu.roll(total, 1, 1))
        values.append(total)
    stacked = jnp.concatenate(split(jnp.concatenate(values, axis=0)), axis=0)
    out = lax.dot_general(
        stacked, slots[...], (((0,), (0,)), ((), ())), preferred_element_type=F32
    )
    for i in range(4):
        out_ref[i] = out[:288, i * 128 : i * 128 + 16]


def program_kernel(
    x_hbm, mom_smem, gamma_smem, out_ref,
    sbuf, gh, gl, w_high, w_low, x_wave, raw_a, raw_b, raw_c, raw_d, yall, pick, mom_all,
    before_buf, move_buf, widen, slots,
    zbuf, dbuf, hbuf, rbuf, spec,
    in_sems, mom_send, mom_recv, pair_send, pair_recv, far_send, far_recv, last_send, last_recv,
):
    gx, gz, ta = (lax.axis_index(name) for name in ("gx", "gz", "ta"))
    core, y_lo, z, y_hi = gz % 2, gz // 2, ta // 2, ta % 2
    y = y_hi * 2 + y_lo
    me = ((z * 4 + y) * 4 + gx) * 2 + core
    chip = (gx * 2 + y_lo) * 8 + ta
    xs = [gx] + [(gx + k) % 4 for k in range(1, 4)]
    ys = [y] + [(y + k) % 4 for k in range(1, 4)]
    zs = [z] + [(z + k) % 4 for k in range(1, 4)]
    cores = [core, 1 - core]
    gzs = [[(value % 2) * 2 + c for c in cores] for value in ys]
    tas = [[at_z * 2 + value // 2 for at_z in zs] for value in ys]
    hops = (0, 1, 2, 1)
    chips = sorted(
        ((dx, dy, dz) for dx in range(4) for dy in range(4) for dz in range(4)),
        key=lambda d: -sum(hops[k] for k in d),
    )

    def device(place, dc=0):
        dx, dy, dz = place
        return (xs[dx], gzs[dy][dc], tas[dy][dz])

    def chip_of(place):
        dx, dy, dz = place
        return (xs[dx] * 2 + ys[dy] % 2) * 8 + tas[dy][dz]

    raws = (raw_a, raw_b, raw_c, raw_d)
    barrier = pltpu.get_barrier_semaphore()
    others = [(place, dc) for place in chips for dc in (0, 1) if place != (0, 0, 0) or dc]
    for place, dc in others:
        pl.semaphore_signal(barrier, inc=1, device_id=device(place, dc), device_id_type=MESH)

    def load(k):
        part = pl.ds(k * 8, 8)
        return pltpu.make_async_copy(x_hbm.at[part], sbuf.at[part], in_sems.at[k])

    for k in range(CHUNKS):
        load(k).start()
    row = jnp.zeros((1, 128), jnp.int32)
    for i in range(4):
        for k in range(4):
            row = jnp.where(iota((1, 128), 1) == 4 * i + k, mom_smem[i, k], row)
    mom_all[me] = row

    fold_high, fold_low = fold_matrix()
    fold_twice = jnp.concatenate([fold_high, fold_high], axis=1)
    fold_rest = jnp.concatenate([fold_low, jnp.zeros_like(fold_low)], axis=1)[64:]

    def fold_step(k, carry):
        load(k).wait()
        for p in range(4):
            pair = k * 4 + p
            both = jnp.concatenate([sbuf[2 * pair], sbuf[2 * pair + 1]], axis=1)
            weights = jnp.concatenate(split(both), axis=0)
            out = jnp.dot(fold_twice, weights, preferred_element_type=F32)
            low = jnp.dot(fold_rest, weights, preferred_element_type=F32)
            out = jnp.concatenate([out[:64], out[64:] + low], axis=0)
            left = out[:, :128].reshape(16, 8, 128)
            right = out[:, 128:].reshape(16, 8, 128)
            high, rest = split(jnp.concatenate([left, right], axis=1))
            rows = pl.ds(pl.multiple_of(pair * 16, 16), 16)
            for q in range(8):
                for part in range(2):
                    lanes = slice(part * 128, part * 128 + 128)
                    gh[q, rows, lanes] = high[2 * q + part]
                    gl[q, rows, lanes] = rest[2 * q + part]
        return carry

    lax.fori_loop(0, 10, fold_step, 0)
    pl.semaphore_wait(barrier, 127)
    for place, dc in others:
        pltpu.make_async_remote_copy(
            src_ref=mom_all.at[me], dst_ref=mom_all.at[me], send_sem=mom_send, recv_sem=mom_recv,
            device_id=device(place, dc), device_id_type=MESH,
        ).start()
    lax.fori_loop(10, CHUNKS, fold_step, 0)

    before_buf[...] = (iota((512, 512), 0) < iota((512, 512), 1)).astype(F32).astype(BF16)
    to_row = iota((512, 512), 1)
    to_chip, to_core, own = to_row >> 3, (to_row >> 2) & 1, to_row & 3
    to_y = (to_chip & 1) * 2 + ((to_chip >> 3) & 1)
    source = own * 128 + ((to_chip >> 1) & 3) * 32 + to_y * 8 + (to_chip >> 4) * 2 + to_core
    move_buf[...] = (source == iota((512, 512), 0)).astype(F32).astype(BF16)
    lane = iota((128, 384), 1)
    source_a = (lane * 2731) >> 16
    source_b = (lane >> 1) - 12 * (((lane >> 1) * 5462) >> 16)
    for k, wanted in enumerate((source_a, source_b)):
        chosen = (iota((128, 384), 0) == wanted).astype(F32).astype(BF16)
        widen[:128, k * 384 : k * 384 + 384] = chosen
        widen[128:, k * 384 : k * 384 + 384] = chosen
    gamma_row = jnp.full((1, 128), -1, jnp.int32)
    for k in range(16):
        gamma_row = jnp.where(iota((1, 128), 1) == k, gamma_smem[k], gamma_row)
    row = iota((128, 128), 0)
    for i in range(4):
        chosen = ((row >> 3) == gamma_row) & ((row & 7) == core * 4 + i)
        chosen = chosen.astype(F32).astype(BF16)
        slots[:128, i * 128 : i * 128 + 128] = chosen
        slots[128:, i * 128 : i * 128 + 128] = chosen
    all_rows = mom_all.at[pl.ds(0, 127)]
    pltpu.make_async_copy(all_rows, all_rows, mom_recv).wait()

    turned = jnp.transpose((mom_all[...].reshape(128, 128) & 31).astype(F32))
    mom = jnp.concatenate([turned[4 * i : 4 * i + 4] for i in range(4)], axis=1)
    mom8 = jnp.concatenate([mom, jnp.zeros_like(mom)], axis=0).astype(BF16)
    mom8 = jnp.dot(mom8, move_buf[...], preferred_element_type=F32)
    ny = mom8[1:2].astype(jnp.int32)
    mom8 = mom8.astype(BF16)
    cls = ((ny >> 1) & 3) + 4 * (ny & 1)
    member = (iota((8, 512), 0) == cls).astype(F32)
    ahead = jnp.dot(member.astype(BF16), before_buf[...], preferred_element_type=F32)
    slot = jnp.sum(member * ahead, axis=0, keepdims=True)
    ends = []
    start = jnp.int32(0)
    for q in range(8):
        count = jnp.sum(member[q : q + 1]).astype(jnp.int32)
        slot = slot + member[q : q + 1] * (start * 128).astype(F32)
        start = start + ((count + 127) >> 7)
        ends.append(start)
    slot = slot.astype(jnp.int32)
    def prepare(j):
        here = (iota((128, 512), 0) + j * 128 == slot).astype(F32).astype(BF16)
        pick[pl.ds(pl.multiple_of(j * 128, 128), 128)] = here
        sorted_mom = lax.dot_general(mom8, here, NT, preferred_element_type=F32).astype(jnp.int32)
        nx, ny, nz, nt = (sorted_mom[i : i + 1] for i in range(4))
        site = iota((32, 128), 0)
        zr, zi = wave(nz * (site >> 2) + nt * (site & 3))
        yr, yi = wave(ny * iota((8, 128), 0))
        pr = jnp.concatenate([zr * yr[k : k + 1] - zi * yi[k : k + 1] for k in range(4)], 0)
        pi = jnp.concatenate([zr * yi[k : k + 1] + zi * yr[k : k + 1] for k in range(4)], 0)
        (prh, prl), (pih, pil) = split(pr), split(pi)
        w_high[j] = jnp.concatenate(
            [jnp.concatenate([prh, pih], 1), jnp.concatenate([-pih, prh], 1)], 0
        )
        w_low[j] = jnp.concatenate(
            [jnp.concatenate([prl, pil], 1), jnp.concatenate([-pil, prl], 1)], 0
        )
        xr, xi = wave(nx * (gx * 8 + iota((8, 128), 0)) + nz * (gz * 8) + nt * (ta * 4))
        x_wave[j, 0] = xr
        x_wave[j, 1] = xi

    def multiply(j, half):
        q = jnp.int32(0)
        for end in ends[:7]:
            q = q + (end <= j).astype(jnp.int32)
        rows = pl.ds(half * HALF * 8, HALF * 8)
        high = gh[q, rows]
        top = w_high[j]
        return (
            jnp.dot(high, top, preferred_element_type=F32)
            + jnp.dot(gl[q, rows], top, preferred_element_type=F32)
            + jnp.dot(high, w_low[j], preferred_element_type=F32)
        )

    def finish(raw, j, half):
        xr, xi = x_wave[j, 0], x_wave[j, 1]
        re = raw[:, :128].reshape(HALF, 8, 128)
        im = raw[:, 128:].reshape(HALF, 8, 128)
        lanes = pl.ds(pl.multiple_of(j * 128, 128), 128)
        for part, value in enumerate((re * xr - im * xi, re * xi + im * xr)):
            first, rest = split(sum_over_x(value))
            yall[half, pl.ds(part * HALF, HALF), lanes] = first
            yall[half, pl.ds((2 + part) * HALF, HALF), lanes] = rest

    def four_tiles(half):
        def step(i, carry):
            first = [multiply(4 * i + k, half) for k in (0, 1)]
            for k in (2, 3):
                finish(raws[k], (4 * i + k + 2 * TILES - 2) % (TILES + 1), half)
            if half == 0:
                prepare(4 * i + 4)
                prepare(4 * i + 5)
            for k in (0, 1):
                raws[k][...] = first[k]
            second = [multiply(4 * i + k, half) for k in (2, 3)]
            for k in (0, 1):
                finish(raws[k], 4 * i + k, half)
            if half == 0:
                prepare(4 * i + 6)
                prepare(4 * i + 7)
            for k in (2, 3):
                raws[k][...] = second[k - 2]
            return carry

        return step

    def to_partner(half):
        return pltpu.make_async_remote_copy(
            src_ref=zbuf.at[half, 1 - core], dst_ref=dbuf.at[half],
            send_sem=pair_send.at[half], recv_sem=pair_recv.at[half],
            device_id=device((0, 0, 0), 1), device_id_type=MESH,
        )

    def restore(half):
        finish(raws[2], TILES - 1, half)
        back = jnp.dot(
            yall[half, :, : TILES * 128], pick[: TILES * 128], preferred_element_type=F32
        )
        back = back[: 2 * HALF] + back[2 * HALF :]
        fill = jnp.zeros((128 - HALF, 512), F32)
        for part in range(2):
            rows = jnp.concatenate([back[part * HALF : (part + 1) * HALF], fill], axis=0)
            zbuf[half, part] = jnp.transpose(rows)
        to_partner(half).start()

    def send_far(half):
        to_partner(half).wait_recv()
        total = (zbuf[half, core] + dbuf[half]) * (1.0 / math.sqrt(float(LX * LY * LZ * LT)))
        hbuf[half] = total.reshape(64, 8, 128)
        rbuf[half, chip] = hbuf[half, chip]
        for place in chips[:-1]:
            pltpu.make_async_remote_copy(
                src_ref=hbuf.at[half, chip_of(place)], dst_ref=rbuf.at[half, chip],
                send_sem=far_send.at[half], recv_sem=far_recv.at[half],
                device_id=device(place), device_id_type=MESH,
            ).start()

    def wait_far(half):
        blocks = rbuf.at[half, pl.ds(0, 63)]
        pltpu.make_async_copy(blocks, blocks, far_recv.at[half]).wait()
        spec[core, half] = jnp.sum(rbuf[half], axis=0)

    for k in range(4):
        prepare(jnp.int32(k))
    lax.fori_loop(0, 3, four_tiles(0), 0)
    restore(0)
    lax.fori_loop(0, 2, four_tiles(1), 0)
    send_far(0)
    lax.fori_loop(2, 3, four_tiles(1), 0)
    restore(1)
    send_far(1)
    wait_far(0)
    wait_far(1)
    last = pltpu.make_async_remote_copy(
        src_ref=spec.at[core], dst_ref=spec.at[core], send_sem=last_send, recv_sem=last_recv,
        device_id=device((0, 0, 0), 1), device_id_type=MESH,
    )
    last.start()
    pltpu.make_async_copy(all_rows, all_rows, mom_send).wait()
    for half in range(2):
        to_partner(half).wait_send()
        blocks = hbuf.at[half, pl.ds(0, 63)]
        pltpu.make_async_copy(blocks, blocks, far_send.at[half]).wait()
    last.wait()
    write_vertices(spec, widen, slots, out_ref)


def vertices_kernel_call(x, momenta, gamma_index):
    vmem = pl.BlockSpec(memory_space=pltpu.VMEM)
    dma = pltpu.SemaphoreType.DMA
    return pl.pallas_call(
        program_kernel,
        out_shape=pltpu.VMEM((4, 288, 16), F32),
        in_specs=[pl.BlockSpec(memory_space=pl.ANY)]
        + [pl.BlockSpec(memory_space=pltpu.SMEM)] * 2,
        out_specs=vmem,
        scratch_shapes=[
            pltpu.VMEM((144, 128, 128), F32),
            pltpu.VMEM((8, 1152, 256), BF16),
            pltpu.VMEM((8, 1152, 256), BF16),
            pltpu.VMEM((TILES + 5, 256, 256), BF16),
            pltpu.VMEM((TILES + 5, 256, 256), BF16),
            pltpu.VMEM((TILES + 5, 2, 8, 128), F32),
            *[pltpu.VMEM((HALF * 8, 256), F32)] * 4,
            pltpu.VMEM((2, 4 * HALF, (TILES + 1) * 128), BF16),
            pltpu.VMEM(((TILES + 5) * 128, 512), BF16),
            pltpu.VMEM((128, 1, 128), jnp.int32),
            pltpu.VMEM((512, 512), BF16),
            pltpu.VMEM((512, 512), BF16),
            pltpu.VMEM((256, 768), BF16),
            pltpu.VMEM((256, 512), BF16),
            pltpu.VMEM((2, 2, 512, 128), F32),
            pltpu.VMEM((2, 512, 128), F32),
            pltpu.VMEM((2, 64, 8, 128), F32),
            pltpu.VMEM((2, 64, 8, 128), F32),
            pltpu.VMEM((2, 2, 8, 128), F32),
            dma((CHUNKS,)),
            dma, dma, dma((2,)), dma((2,)), dma((2,)), dma((2,)), dma, dma,
        ],
        compiler_params=pltpu.CompilerParams(
            collective_id=0, has_side_effects=True, vmem_limit_bytes=56 * 1024 * 1024
        ),
    )(x, momenta, gamma_index)


def site_major(propagator):
    x = jnp.transpose(propagator, (1, 2, 0, 3)).reshape(144, 2, 64, 128)
    return jnp.transpose(x, (0, 2, 1, 3)).reshape(144, 128, 128)


def body(propagator, momenta, gamma_index):
    out = vertices_kernel_call(site_major(propagator), momenta, gamma_index)
    return jnp.transpose(out.reshape(4, 12, 12, 2, 16), (0, 4, 3, 1, 2))


def solution(mesh):
    placed = (P(None, None, None, ("gx", "gz", "ta")), P(("gx", "gz", "ta"), None), P())
    return jax.shard_map(
        body,
        mesh=mesh,
        in_specs=placed,
        out_specs=P(("gx", "gz", "ta"), None, None, None, None),
        check_vma=False,
    )
```

```python
import math

import jax
import jax.numpy as jnp
import numpy as np
from jax import lax
from jax.experimental import pallas as pl
from jax.experimental.pallas import tpu as pltpu
from jax.sharding import PartitionSpec as P

LX = LY = LZ = LT = 32
MESH = pl.DeviceIdType.MESH
F32 = jnp.float32
BF16 = jnp.bfloat16
TILES = 11
CHUNKS = 18
HALF = 72


def split(value):
    high = value.astype(BF16)
    return high, (value - high.astype(F32)).astype(BF16)


def sine(index):
    turn = ((index + 16) & 31) - 16
    turn = jnp.where(turn > 8, 16 - turn, jnp.where(turn < -8, -16 - turn, turn))
    u = turn.astype(F32) * (math.pi / 16)
    s = u * u
    poly = 1 / 362880 - s * (1 / 39916800)
    for factor in (-1 / 5040, 1 / 120, -1 / 6, 1.0):
        poly = factor + s * poly
    return u * poly


def wave(index):
    return sine(index + 8), -sine(index)


def sum_over_x(value):
    groups = value.shape[0] // 8
    value = value.reshape(groups, 8, 8, 128)
    sub = lax.broadcasted_iota(jnp.int32, (8, 128), 0)
    for step in (4, 2, 1):
        keep = (sub & step) == 0
        out = []
        for k in range(step):
            a, b = value[:, k], value[:, k + step]
            rolled_a = pltpu.roll(a, 8 - step, 1)
            rolled_b = pltpu.roll(b, step, 1)
            out.append(jnp.where(keep, a, rolled_b) + jnp.where(keep, rolled_a, b))
        value = jnp.stack(out, axis=1)
    return value.reshape(groups * 8, 128)


NT = (((1,), (1,)), ((), ()))


def iota(shape, dim):
    return lax.broadcasted_iota(jnp.int32, shape, dim)


def fold_matrix():
    row, col = iota((128, 128), 0), iota((128, 128), 1)
    q = row >> 4
    number = jnp.where(q < 4, 2 * q, 2 * q - 7)
    re, im = wave(4 * number * ((col >> 1) & 7))
    from_im, to_im = (col & 1) == 1, ((row >> 3) & 1) == 1
    value = jnp.where(from_im == to_im, re, jnp.where(to_im, im, -im))
    return split(jnp.where((row & 7) == (col >> 4), value, 0.0))


def clifford_table():
    zeros = np.zeros((4, 4))
    first = (zeros, np.array([[0, 0, 0, 1], [0, 0, 1, 0], [0, -1, 0, 0], [-1, 0, 0, 0]]))
    second = (np.array([[0, 0, 0, -1], [0, 0, 1, 0], [0, 1, 0, 0], [-1, 0, 0, 0]]), zeros)
    third = (zeros, np.array([[0, 0, 1, 0], [0, 0, 0, -1], [-1, 0, 0, 0], [0, 1, 0, 0]]))
    fourth = (np.array([[0, 0, 1, 0], [0, 0, 0, 1], [1, 0, 0, 0], [0, 1, 0, 0]]), zeros)
    basis = [first, second, third, fourth]
    tables_re = []
    tables_im = []
    for mask in range(16):
        matrix_re = np.identity(4)
        matrix_im = np.zeros((4, 4))
        for bit in range(4):
            if mask >> bit & 1:
                basis_re, basis_im = basis[bit]
                new_re = matrix_re @ basis_re - matrix_im @ basis_im
                new_im = matrix_re @ basis_im + matrix_im @ basis_re
                matrix_re, matrix_im = (new_re, new_im)
        tables_re.append(matrix_re)
        tables_im.append(matrix_im)
    return (np.stack(tables_re), np.stack(tables_im))


def structures():
    table_re, table_im = clifford_table()
    out = []
    for re, im in zip(table_re, table_im, strict=True):
        matrix = im if im.any() else re
        columns = [int(np.flatnonzero(line)[0]) for line in matrix]
        signs = [float(line[k]) for line, k in zip(matrix, columns, strict=True)]
        out.append((bool(im.any()), columns, signs))
    return out


def write_vertices(spec, widen, slots, out_ref):
    keep = iota((8, 128), 1) < HALF
    lines = []
    for sink in range(12):
        half, k = divmod(sink, 6)
        for part in range(2):
            line = jnp.where(keep, spec[part, half], 0.0)
            lines.append(pltpu.roll(line, 128 - 12 * k, 1) if k else line)
    wide = jnp.concatenate(split(jnp.concatenate(lines, axis=0)), axis=1)
    wide = jnp.dot(wide, widen[...], preferred_element_type=F32)
    even = (iota((8, 384), 1) & 1) == 0
    left_re = [wide[16 * k : 16 * k + 8, :384] for k in range(12)]
    left_im = [wide[16 * k + 8 : 16 * k + 16, :384] for k in range(12)]
    right, turned = [], []
    for k in range(12):
        re, im = wide[16 * k : 16 * k + 8, 384:], wide[16 * k + 8 : 16 * k + 16, 384:]
        right.append(jnp.where(even, re, im))
        turned.append(jnp.where(even, im, -re))

    def pair(s, t):
        total = None
        for c in range(3):
            a, b = 3 * s + c, 3 * t + c
            term = left_re[a] * right[b] + left_im[a] * turned[b]
            total = term if total is None else total + term
        return total

    pairs = {}
    values = []
    for imaginary, columns, signs in structures():
        total = None
        for s in range(4):
            if (s, columns[s]) not in pairs:
                pairs[s, columns[s]] = pair(s, columns[s])
            term = pairs[s, columns[s]]
            if total is None:
                total = term if signs[s] > 0 else -term
            else:
                total = total + term if signs[s] > 0 else total - term
        if imaginary:
            total = jnp.where(even, -pltpu.roll(total, 383, 1), pltpu.roll(total, 1, 1))
        values.append(total)
    stacked = jnp.concatenate(split(jnp.concatenate(values, axis=0)), axis=0)
    out = lax.dot_general(
        stacked, slots[...], (((0,), (0,)), ((), ())), preferred_element_type=F32
    )
    for i in range(4):
        out_ref[i] = out[:288, i * 128 : i * 128 + 16]


def program_kernel(
    x_hbm, mom_smem, gamma_smem, out_ref,
    sbuf, gh, gl, w_high, w_low, x_wave, raw_a, raw_b, raw_c, raw_d, yall, pick, mom_all,
    before_buf, move_buf, widen, slots,
    zbuf, dbuf, hbuf, rbuf, spec,
    in_sems, mom_send, mom_recv, pair_send, pair_recv, far_send, far_recv, last_send, last_recv,
):
    gx, gz, ta = (lax.axis_index(name) for name in ("gx", "gz", "ta"))
    core, y_lo, z, y_hi = gz % 2, gz // 2, ta // 2, ta % 2
    y = y_hi * 2 + y_lo
    me = ((z * 4 + y) * 4 + gx) * 2 + core
    chip = (gx * 2 + y_lo) * 8 + ta
    xs = [gx] + [(gx + k) % 4 for k in range(1, 4)]
    ys = [y] + [(y + k) % 4 for k in range(1, 4)]
    zs = [z] + [(z + k) % 4 for k in range(1, 4)]
    cores = [core, 1 - core]
    gzs = [[(value % 2) * 2 + c for c in cores] for value in ys]
    tas = [[at_z * 2 + value // 2 for at_z in zs] for value in ys]
    hops = (0, 1, 2, 1)
    chips = sorted(
        ((dx, dy, dz) for dx in range(4) for dy in range(4) for dz in range(4)),
        key=lambda d: -sum(hops[k] for k in d),
    )

    def device(place, dc=0):
        dx, dy, dz = place
        return (xs[dx], gzs[dy][dc], tas[dy][dz])

    def chip_of(place):
        dx, dy, dz = place
        return (xs[dx] * 2 + ys[dy] % 2) * 8 + tas[dy][dz]

    raws = (raw_a, raw_b, raw_c, raw_d)
    barrier = pltpu.get_barrier_semaphore()
    others = [(place, dc) for place in chips for dc in (0, 1) if place != (0, 0, 0) or dc]
    for place, dc in others:
        pl.semaphore_signal(barrier, inc=1, device_id=device(place, dc), device_id_type=MESH)

    def load(k):
        part = pl.ds(k * 8, 8)
        return pltpu.make_async_copy(x_hbm.at[part], sbuf.at[part], in_sems.at[k])

    for k in range(CHUNKS):
        load(k).start()
    row = jnp.zeros((1, 128), jnp.int32)
    for i in range(4):
        for k in range(4):
            row = jnp.where(iota((1, 128), 1) == 4 * i + k, mom_smem[i, k], row)
    mom_all[me] = row

    fold_high, fold_low = fold_matrix()
    fold_twice = jnp.concatenate([fold_high, fold_high], axis=1)
    fold_rest = jnp.concatenate([fold_low, jnp.zeros_like(fold_low)], axis=1)[64:]

    def fold_step(k, carry):
        load(k).wait()
        for p in range(4):
            pair = k * 4 + p
            both = jnp.concatenate([sbuf[2 * pair], sbuf[2 * pair + 1]], axis=1)
            weights = jnp.concatenate(split(both), axis=0)
            out = jnp.dot(fold_twice, weights, preferred_element_type=F32)
            low = jnp.dot(fold_rest, weights, preferred_element_type=F32)
            out = jnp.concatenate([out[:64], out[64:] + low], axis=0)
            left = out[:, :128].reshape(16, 8, 128)
            right = out[:, 128:].reshape(16, 8, 128)
            high, rest = split(jnp.concatenate([left, right], axis=1))
            rows = pl.ds(pl.multiple_of(pair * 16, 16), 16)
            for q in range(8):
                for part in range(2):
                    lanes = slice(part * 128, part * 128 + 128)
                    gh[q, rows, lanes] = high[2 * q + part]
                    gl[q, rows, lanes] = rest[2 * q + part]
        return carry

    lax.fori_loop(0, 10, fold_step, 0)
    pl.semaphore_wait(barrier, 127)
    for place, dc in others:
        pltpu.make_async_remote_copy(
            src_ref=mom_all.at[me], dst_ref=mom_all.at[me], send_sem=mom_send, recv_sem=mom_recv,
            device_id=device(place, dc), device_id_type=MESH,
        ).start()
    lax.fori_loop(10, CHUNKS, fold_step, 0)

    before_buf[...] = (iota((512, 512), 0) < iota((512, 512), 1)).astype(F32).astype(BF16)
    to_row = iota((512, 512), 1)
    to_chip, to_core, own = to_row >> 3, (to_row >> 2) & 1, to_row & 3
    to_y = (to_chip & 1) * 2 + ((to_chip >> 3) & 1)
    source = own * 128 + ((to_chip >> 1) & 3) * 32 + to_y * 8 + (to_chip >> 4) * 2 + to_core
    move_buf[...] = (source == iota((512, 512), 0)).astype(F32).astype(BF16)
    lane = iota((128, 384), 1)
    source_a = (lane * 2731) >> 16
    source_b = (lane >> 1) - 12 * (((lane >> 1) * 5462) >> 16)
    for k, wanted in enumerate((source_a, source_b)):
        chosen = (iota((128, 384), 0) == wanted).astype(F32).astype(BF16)
        widen[:128, k * 384 : k * 384 + 384] = chosen
        widen[128:, k * 384 : k * 384 + 384] = chosen
    gamma_row = jnp.full((1, 128), -1, jnp.int32)
    for k in range(16):
        gamma_row = jnp.where(iota((1, 128), 1) == k, gamma_smem[k], gamma_row)
    row = iota((128, 128), 0)
    for i in range(4):
        chosen = ((row >> 3) == gamma_row) & ((row & 7) == core * 4 + i)
        chosen = chosen.astype(F32).astype(BF16)
        slots[:128, i * 128 : i * 128 + 128] = chosen
        slots[128:, i * 128 : i * 128 + 128] = chosen
    all_rows = mom_all.at[pl.ds(0, 127)]
    pltpu.make_async_copy(all_rows, all_rows, mom_recv).wait()

    turned = jnp.transpose((mom_all[...].reshape(128, 128) & 31).astype(F32))
    mom = jnp.concatenate([turned[4 * i : 4 * i + 4] for i in range(4)], axis=1)
    mom8 = jnp.concatenate([mom, jnp.zeros_like(mom)], axis=0).astype(BF16)
    mom8 = jnp.dot(mom8, move_buf[...], preferred_element_type=F32)
    ny = mom8[1:2].astype(jnp.int32)
    mom8 = mom8.astype(BF16)
    cls = ((ny >> 1) & 3) + 4 * (ny & 1)
    member = (iota((8, 512), 0) == cls).astype(F32)
    ahead = jnp.dot(member.astype(BF16), before_buf[...], preferred_element_type=F32)
    slot = jnp.sum(member * ahead, axis=0, keepdims=True)
    ends = []
    start = jnp.int32(0)
    for q in range(8):
        count = jnp.sum(member[q : q + 1]).astype(jnp.int32)
        slot = slot + member[q : q + 1] * (start * 128).astype(F32)
        start = start + ((count + 127) >> 7)
        ends.append(start)
    slot = slot.astype(jnp.int32)
    def prepare(j):
        here = (iota((128, 512), 0) + j * 128 == slot).astype(F32).astype(BF16)
        pick[pl.ds(pl.multiple_of(j * 128, 128), 128)] = here
        sorted_mom = lax.dot_general(mom8, here, NT, preferred_element_type=F32).astype(jnp.int32)
        nx, ny, nz, nt = (sorted_mom[i : i + 1] for i in range(4))
        k, r = iota((16, 128), 0), iota((8, 128), 0)
        phases = (
            nz * (r >> 2) + nt * (r & 3),
            ny * (k >> 2) + nz * (2 * (k & 3)),
            nx * (gx * 8 + r) + nz * (gz * 8) + nt * (ta * 4),
        )
        re, im = wave(jnp.concatenate(phases, axis=0))
        lr, li = re[:8], im[:8]
        rows = [(re[n : n + 1], im[n : n + 1]) for n in range(8, 24)]
        pr = jnp.concatenate([lr * hr - li * hi for hr, hi in rows], 0)
        pi = jnp.concatenate([lr * hi + li * hr for hr, hi in rows], 0)
        (prh, prl), (pih, pil) = split(pr), split(pi)
        w_high[j] = jnp.concatenate(
            [jnp.concatenate([prh, pih], 1), jnp.concatenate([-pih, prh], 1)], 0
        )
        w_low[j] = jnp.concatenate(
            [jnp.concatenate([prl, pil], 1), jnp.concatenate([-pil, prl], 1)], 0
        )
        x_wave[j, 0] = re[24:]
        x_wave[j, 1] = im[24:]

    def multiply(j, half):
        q = jnp.int32(0)
        for end in ends[:7]:
            q = q + (end <= j).astype(jnp.int32)
        rows = pl.ds(half * HALF * 8, HALF * 8)
        high = gh[q, rows]
        top = w_high[j]
        return (
            jnp.dot(high, top, preferred_element_type=F32)
            + jnp.dot(gl[q, rows], top, preferred_element_type=F32)
            + jnp.dot(high, w_low[j], preferred_element_type=F32)
        )

    def finish(raw, j, half):
        xr, xi = x_wave[j, 0], x_wave[j, 1]
        re = raw[:, :128].reshape(HALF, 8, 128)
        im = raw[:, 128:].reshape(HALF, 8, 128)
        lanes = pl.ds(pl.multiple_of(j * 128, 128), 128)
        for part, value in enumerate((re * xr - im * xi, re * xi + im * xr)):
            first, rest = split(sum_over_x(value))
            yall[half, pl.ds(part * HALF, HALF), lanes] = first
            yall[half, pl.ds((2 + part) * HALF, HALF), lanes] = rest

    def four_tiles(i, half, ahead):
        out = [multiply(4 * i + k, half) for k in (0, 1)]
        for k in (2, 3):
            finish(raws[k], (4 * i + k + 2 * TILES - 2) % (TILES + 1), half)
        if ahead:
            prepare(4 * i + 4)
            prepare(4 * i + 5)
        for k in (0, 1):
            raws[k][...] = out[k]
        out = [multiply(4 * i + k, half) for k in (2, 3)]
        for k in (0, 1):
            finish(raws[k], 4 * i + k, half)
        if ahead:
            prepare(4 * i + 6)
            prepare(4 * i + 7)
        for k in (2, 3):
            raws[k][...] = out[k - 2]

    def tiles_loop(half):
        def step(i, carry):
            four_tiles(i, half, half == 0)
            return carry

        lax.fori_loop(0, 2, step, 0)

    def to_partner(half):
        return pltpu.make_async_remote_copy(
            src_ref=zbuf.at[half, 1 - core], dst_ref=dbuf.at[half],
            send_sem=pair_send.at[half], recv_sem=pair_recv.at[half],
            device_id=device((0, 0, 0), 1), device_id_type=MESH,
        )

    def restore(half):
        finish(raws[2], TILES - 1, half)
        back = jnp.dot(
            yall[half, :, : TILES * 128], pick[: TILES * 128], preferred_element_type=F32
        )
        back = back[: 2 * HALF] + back[2 * HALF :]
        fill = jnp.zeros((128 - HALF, 512), F32)
        for part in range(2):
            rows = jnp.concatenate([back[part * HALF : (part + 1) * HALF], fill], axis=0)
            zbuf[half, part] = jnp.transpose(rows)
        to_partner(half).start()

    def send_far(half):
        to_partner(half).wait_recv()
        total = (zbuf[half, core] + dbuf[half]) * (1.0 / math.sqrt(float(LX * LY * LZ * LT)))
        hbuf[half] = total.reshape(64, 8, 128)
        rbuf[half, chip] = hbuf[half, chip]
        for place in chips[:-1]:
            pltpu.make_async_remote_copy(
                src_ref=hbuf.at[half, chip_of(place)], dst_ref=rbuf.at[half, chip],
                send_sem=far_send.at[half], recv_sem=far_recv.at[half],
                device_id=device(place), device_id_type=MESH,
            ).start()

    def wait_far(half):
        blocks = rbuf.at[half, pl.ds(0, 63)]
        pltpu.make_async_copy(blocks, blocks, far_recv.at[half]).wait()
        spec[core, half] = jnp.sum(rbuf[half], axis=0)

    for k in range(4):
        prepare(jnp.int32(k))
    tiles_loop(0)
    four_tiles(2, 0, False)
    restore(0)
    tiles_loop(1)
    send_far(0)
    four_tiles(2, 1, False)
    restore(1)
    send_far(1)
    wait_far(0)
    wait_far(1)
    last = pltpu.make_async_remote_copy(
        src_ref=spec.at[core], dst_ref=spec.at[core], send_sem=last_send, recv_sem=last_recv,
        device_id=device((0, 0, 0), 1), device_id_type=MESH,
    )
    last.start()
    pltpu.make_async_copy(all_rows, all_rows, mom_send).wait()
    for half in range(2):
        to_partner(half).wait_send()
        blocks = hbuf.at[half, pl.ds(0, 63)]
        pltpu.make_async_copy(blocks, blocks, far_send.at[half]).wait()
    last.wait()
    write_vertices(spec, widen, slots, out_ref)


def vertices_kernel_call(x, momenta, gamma_index):
    vmem = pl.BlockSpec(memory_space=pltpu.VMEM)
    dma = pltpu.SemaphoreType.DMA
    return pl.pallas_call(
        program_kernel,
        out_shape=pltpu.VMEM((4, 288, 16), F32),
        in_specs=[pl.BlockSpec(memory_space=pl.ANY)]
        + [pl.BlockSpec(memory_space=pltpu.SMEM)] * 2,
        out_specs=vmem,
        scratch_shapes=[
            pltpu.VMEM((144, 128, 128), F32),
            pltpu.VMEM((8, 1152, 256), BF16),
            pltpu.VMEM((8, 1152, 256), BF16),
            pltpu.VMEM((TILES + 1, 256, 256), BF16),
            pltpu.VMEM((TILES + 1, 256, 256), BF16),
            pltpu.VMEM((TILES + 1, 2, 8, 128), F32),
            *[pltpu.VMEM((HALF * 8, 256), F32)] * 4,
            pltpu.VMEM((2, 4 * HALF, (TILES + 1) * 128), BF16),
            pltpu.VMEM(((TILES + 1) * 128, 512), BF16),
            pltpu.VMEM((128, 1, 128), jnp.int32),
            pltpu.VMEM((512, 512), BF16),
            pltpu.VMEM((512, 512), BF16),
            pltpu.VMEM((256, 768), BF16),
            pltpu.VMEM((256, 512), BF16),
            pltpu.VMEM((2, 2, 512, 128), F32),
            pltpu.VMEM((2, 512, 128), F32),
            pltpu.VMEM((2, 64, 8, 128), F32),
            pltpu.VMEM((2, 64, 8, 128), F32),
            pltpu.VMEM((2, 2, 8, 128), F32),
            dma((CHUNKS,)),
            dma, dma, dma((2,)), dma((2,)), dma((2,)), dma((2,)), dma, dma,
        ],
        compiler_params=pltpu.CompilerParams(
            collective_id=0, has_side_effects=True, vmem_limit_bytes=56 * 1024 * 1024
        ),
    )(x, momenta, gamma_index)


def site_major(propagator):
    x = jnp.transpose(propagator, (1, 2, 0, 3)).reshape(144, 2, 64, 128)
    return jnp.transpose(x, (0, 2, 1, 3)).reshape(144, 128, 128)


def body(propagator, momenta, gamma_index):
    out = vertices_kernel_call(site_major(propagator), momenta, gamma_index)
    return jnp.transpose(out.reshape(4, 12, 12, 2, 16), (0, 4, 3, 1, 2))


def solution(mesh):
    placed = (P(None, None, None, ("gx", "gz", "ta")), P(("gx", "gz", "ta"), None), P())
    return jax.shard_map(
        body,
        mesh=mesh,
        in_specs=placed,
        out_specs=P(("gx", "gz", "ta"), None, None, None, None),
        check_vma=False,
    )
```

```python
import math

import jax
import jax.numpy as jnp
import numpy as np
from jax import lax
from jax.experimental import pallas as pl
from jax.experimental.pallas import tpu as pltpu
from jax.sharding import PartitionSpec as P

LX = LY = LZ = LT = 32
MESH = pl.DeviceIdType.MESH
F32 = jnp.float32
BF16 = jnp.bfloat16
TILES = 11
CHUNKS = 18
HALF = 72


def split(value):
    high = value.astype(BF16)
    return high, (value - high.astype(F32)).astype(BF16)


def sine(index):
    turn = ((index + 16) & 31) - 16
    turn = jnp.where(turn > 8, 16 - turn, jnp.where(turn < -8, -16 - turn, turn))
    u = turn.astype(F32) * (math.pi / 16)
    s = u * u
    poly = 1 / 362880 - s * (1 / 39916800)
    for factor in (-1 / 5040, 1 / 120, -1 / 6, 1.0):
        poly = factor + s * poly
    return u * poly


def wave(index):
    return sine(index + 8), -sine(index)


def sum_over_x(value):
    groups = value.shape[0] // 8
    value = value.reshape(groups, 8, 8, 128)
    sub = lax.broadcasted_iota(jnp.int32, (8, 128), 0)
    for step in (4, 2, 1):
        keep = (sub & step) == 0
        out = []
        for k in range(step):
            a, b = value[:, k], value[:, k + step]
            rolled_a = pltpu.roll(a, 8 - step, 1)
            rolled_b = pltpu.roll(b, step, 1)
            out.append(jnp.where(keep, a, rolled_b) + jnp.where(keep, rolled_a, b))
        value = jnp.stack(out, axis=1)
    return value.reshape(groups * 8, 128)


NT = (((1,), (1,)), ((), ()))


def iota(shape, dim):
    return lax.broadcasted_iota(jnp.int32, shape, dim)


def fold_matrix():
    row, col = iota((128, 128), 0), iota((128, 128), 1)
    q = row >> 4
    number = jnp.where(q < 4, 2 * q, 2 * q - 7)
    re, im = wave(4 * number * ((col >> 1) & 7))
    from_im, to_im = (col & 1) == 1, ((row >> 3) & 1) == 1
    value = jnp.where(from_im == to_im, re, jnp.where(to_im, im, -im))
    return split(jnp.where((row & 7) == (col >> 4), value, 0.0))


def clifford_table():
    zeros = np.zeros((4, 4))
    first = (zeros, np.array([[0, 0, 0, 1], [0, 0, 1, 0], [0, -1, 0, 0], [-1, 0, 0, 0]]))
    second = (np.array([[0, 0, 0, -1], [0, 0, 1, 0], [0, 1, 0, 0], [-1, 0, 0, 0]]), zeros)
    third = (zeros, np.array([[0, 0, 1, 0], [0, 0, 0, -1], [-1, 0, 0, 0], [0, 1, 0, 0]]))
    fourth = (np.array([[0, 0, 1, 0], [0, 0, 0, 1], [1, 0, 0, 0], [0, 1, 0, 0]]), zeros)
    basis = [first, second, third, fourth]
    tables_re = []
    tables_im = []
    for mask in range(16):
        matrix_re = np.identity(4)
        matrix_im = np.zeros((4, 4))
        for bit in range(4):
            if mask >> bit & 1:
                basis_re, basis_im = basis[bit]
                new_re = matrix_re @ basis_re - matrix_im @ basis_im
                new_im = matrix_re @ basis_im + matrix_im @ basis_re
                matrix_re, matrix_im = (new_re, new_im)
        tables_re.append(matrix_re)
        tables_im.append(matrix_im)
    return (np.stack(tables_re), np.stack(tables_im))


def structures():
    table_re, table_im = clifford_table()
    out = []
    for re, im in zip(table_re, table_im, strict=True):
        matrix = im if im.any() else re
        columns = [int(np.flatnonzero(line)[0]) for line in matrix]
        signs = [float(line[k]) for line, k in zip(matrix, columns, strict=True)]
        out.append((bool(im.any()), columns, signs))
    return out


def write_vertices(spec, widen, slots, out_ref):
    keep = iota((8, 128), 1) < HALF
    lines = []
    for sink in range(12):
        half, k = divmod(sink, 6)
        for part in range(2):
            line = jnp.where(keep, spec[part, half], 0.0)
            lines.append(pltpu.roll(line, 128 - 12 * k, 1) if k else line)
    wide = jnp.concatenate(split(jnp.concatenate(lines, axis=0)), axis=1)
    wide = jnp.dot(wide, widen[...], preferred_element_type=F32)
    even = (iota((8, 384), 1) & 1) == 0
    left_re = [wide[16 * k : 16 * k + 8, :384] for k in range(12)]
    left_im = [wide[16 * k + 8 : 16 * k + 16, :384] for k in range(12)]
    right, turned = [], []
    for k in range(12):
        re, im = wide[16 * k : 16 * k + 8, 384:], wide[16 * k + 8 : 16 * k + 16, 384:]
        right.append(jnp.where(even, re, im))
        turned.append(jnp.where(even, im, -re))

    def pair(s, t):
        total = None
        for c in range(3):
            a, b = 3 * s + c, 3 * t + c
            term = left_re[a] * right[b] + left_im[a] * turned[b]
            total = term if total is None else total + term
        return total

    pairs = {}
    values = []
    for imaginary, columns, signs in structures():
        total = None
        for s in range(4):
            if (s, columns[s]) not in pairs:
                pairs[s, columns[s]] = pair(s, columns[s])
            term = pairs[s, columns[s]]
            if total is None:
                total = term if signs[s] > 0 else -term
            else:
                total = total + term if signs[s] > 0 else total - term
        if imaginary:
            total = jnp.where(even, -pltpu.roll(total, 383, 1), pltpu.roll(total, 1, 1))
        values.append(total)
    stacked = jnp.concatenate(split(jnp.concatenate(values, axis=0)), axis=0)
    out = lax.dot_general(
        stacked, slots[...], (((0,), (0,)), ((), ())), preferred_element_type=F32
    )
    for i in range(4):
        out_ref[i] = out[:288, i * 128 : i * 128 + 16]


def program_kernel(
    x_hbm, mom_smem, gamma_smem, out_ref,
    sbuf, gh, gl, w_high, w_low, x_wave, raw_a, raw_b, raw_c, raw_d, yall, pick, mom_all,
    before_buf, move_buf, widen, slots,
    zbuf, dbuf, hbuf, rbuf, own_out, own_in, spec,
    in_sems, mom_send, mom_recv, pair_send, pair_recv, far_send, far_recv, last_send, last_recv,
):
    gx, gz, ta = (lax.axis_index(name) for name in ("gx", "gz", "ta"))
    core, y_lo, z, y_hi = gz % 2, gz // 2, ta // 2, ta % 2
    y = y_hi * 2 + y_lo
    me = ((z * 4 + y) * 4 + gx) * 2 + core
    chip = (gx * 2 + y_lo) * 8 + ta
    xs = [gx] + [(gx + k) % 4 for k in range(1, 4)]
    ys = [y] + [(y + k) % 4 for k in range(1, 4)]
    zs = [z] + [(z + k) % 4 for k in range(1, 4)]
    cores = [core, 1 - core]
    gzs = [[(value % 2) * 2 + c for c in cores] for value in ys]
    tas = [[at_z * 2 + value // 2 for at_z in zs] for value in ys]
    hops = (0, 1, 2, 1)
    chips = sorted(
        ((dx, dy, dz) for dx in range(4) for dy in range(4) for dz in range(4)),
        key=lambda d: -sum(hops[k] for k in d),
    )

    def device(place, dc=0):
        dx, dy, dz = place
        return (xs[dx], gzs[dy][dc], tas[dy][dz])

    def chip_of(place):
        dx, dy, dz = place
        return (xs[dx] * 2 + ys[dy] % 2) * 8 + tas[dy][dz]

    raws = (raw_a, raw_b, raw_c, raw_d)
    barrier = pltpu.get_barrier_semaphore()
    others = [(place, dc) for place in chips for dc in (0, 1) if place != (0, 0, 0) or dc]
    for place, dc in others:
        pl.semaphore_signal(barrier, inc=1, device_id=device(place, dc), device_id_type=MESH)

    def load(k):
        part = pl.ds(k * 8, 8)
        return pltpu.make_async_copy(x_hbm.at[part], sbuf.at[part], in_sems.at[k])

    for k in range(CHUNKS):
        load(k).start()
    row = jnp.zeros((1, 128), jnp.int32)
    for i in range(4):
        for k in range(4):
            row = jnp.where(iota((1, 128), 1) == 4 * i + k, mom_smem[i, k], row)
    mom_all[me] = row

    fold_high, fold_low = fold_matrix()
    fold_twice = jnp.concatenate([fold_high, fold_high], axis=1)
    fold_rest = jnp.concatenate([fold_low, jnp.zeros_like(fold_low)], axis=1)[64:]

    def fold_step(k, carry):
        load(k).wait()
        for p in range(4):
            pair = k * 4 + p
            both = jnp.concatenate([sbuf[2 * pair], sbuf[2 * pair + 1]], axis=1)
            weights = jnp.concatenate(split(both), axis=0)
            out = jnp.dot(fold_twice, weights, preferred_element_type=F32)
            low = jnp.dot(fold_rest, weights, preferred_element_type=F32)
            out = jnp.concatenate([out[:64], out[64:] + low], axis=0)
            left = out[:, :128].reshape(16, 8, 128)
            right = out[:, 128:].reshape(16, 8, 128)
            high, rest = split(jnp.concatenate([left, right], axis=1))
            rows = pl.ds(pl.multiple_of(pair * 16, 16), 16)
            for q in range(8):
                for part in range(2):
                    lanes = slice(part * 128, part * 128 + 128)
                    gh[q, rows, lanes] = high[2 * q + part]
                    gl[q, rows, lanes] = rest[2 * q + part]
        return carry

    lax.fori_loop(0, 10, fold_step, 0)
    pl.semaphore_wait(barrier, 127)
    for place, dc in others:
        pltpu.make_async_remote_copy(
            src_ref=mom_all.at[me], dst_ref=mom_all.at[me], send_sem=mom_send, recv_sem=mom_recv,
            device_id=device(place, dc), device_id_type=MESH,
        ).start()
    lax.fori_loop(10, CHUNKS, fold_step, 0)

    before_buf[...] = (iota((512, 512), 0) < iota((512, 512), 1)).astype(F32).astype(BF16)
    to_row = iota((512, 512), 1)
    to_chip, to_core, own = to_row >> 3, (to_row >> 2) & 1, to_row & 3
    to_y = (to_chip & 1) * 2 + ((to_chip >> 3) & 1)
    source = own * 128 + ((to_chip >> 1) & 3) * 32 + to_y * 8 + (to_chip >> 4) * 2 + to_core
    move_buf[...] = (source == iota((512, 512), 0)).astype(F32).astype(BF16)
    lane = iota((128, 384), 1)
    source_a = (lane * 2731) >> 16
    source_b = (lane >> 1) - 12 * (((lane >> 1) * 5462) >> 16)
    for k, wanted in enumerate((source_a, source_b)):
        chosen = (iota((128, 384), 0) == wanted).astype(F32).astype(BF16)
        widen[:128, k * 384 : k * 384 + 384] = chosen
        widen[128:, k * 384 : k * 384 + 384] = chosen
    gamma_row = jnp.full((1, 128), -1, jnp.int32)
    for k in range(16):
        gamma_row = jnp.where(iota((1, 128), 1) == k, gamma_smem[k], gamma_row)
    row = iota((128, 128), 0)
    for i in range(4):
        chosen = ((row >> 3) == gamma_row) & ((row & 7) == core * 4 + i)
        chosen = chosen.astype(F32).astype(BF16)
        slots[:128, i * 128 : i * 128 + 128] = chosen
        slots[128:, i * 128 : i * 128 + 128] = chosen
    all_rows = mom_all.at[pl.ds(0, 127)]
    pltpu.make_async_copy(all_rows, all_rows, mom_recv).wait()

    turned = jnp.transpose((mom_all[...].reshape(128, 128) & 31).astype(F32))
    mom = jnp.concatenate([turned[4 * i : 4 * i + 4] for i in range(4)], axis=1)
    mom8 = jnp.concatenate([mom, jnp.zeros_like(mom)], axis=0).astype(BF16)
    mom8 = jnp.dot(mom8, move_buf[...], preferred_element_type=F32)
    ny = mom8[1:2].astype(jnp.int32)
    mom8 = mom8.astype(BF16)
    cls = ((ny >> 1) & 3) + 4 * (ny & 1)
    member = (iota((8, 512), 0) == cls).astype(F32)
    ahead = jnp.dot(member.astype(BF16), before_buf[...], preferred_element_type=F32)
    slot = jnp.sum(member * ahead, axis=0, keepdims=True)
    ends = []
    start = jnp.int32(0)
    for q in range(8):
        count = jnp.sum(member[q : q + 1]).astype(jnp.int32)
        slot = slot + member[q : q + 1] * (start * 128).astype(F32)
        start = start + ((count + 127) >> 7)
        ends.append(start)
    slot = slot.astype(jnp.int32)
    def prepare(j):
        here = (iota((128, 512), 0) + j * 128 == slot).astype(F32).astype(BF16)
        pick[pl.ds(pl.multiple_of(j * 128, 128), 128)] = here
        sorted_mom = lax.dot_general(mom8, here, NT, preferred_element_type=F32).astype(jnp.int32)
        nx, ny, nz, nt = (sorted_mom[i : i + 1] for i in range(4))
        k, r = iota((16, 128), 0), iota((8, 128), 0)
        phases = (
            nz * (r >> 2) + nt * (r & 3),
            ny * (k >> 2) + nz * (2 * (k & 3)),
            nx * (gx * 8 + r) + nz * (gz * 8) + nt * (ta * 4),
        )
        re, im = wave(jnp.concatenate(phases, axis=0))
        lr, li = re[:8], im[:8]
        rows = [(re[n : n + 1], im[n : n + 1]) for n in range(8, 24)]
        pr = jnp.concatenate([lr * hr - li * hi for hr, hi in rows], 0)
        pi = jnp.concatenate([lr * hi + li * hr for hr, hi in rows], 0)
        (prh, prl), (pih, pil) = split(pr), split(pi)
        w_high[j] = jnp.concatenate(
            [jnp.concatenate([prh, pih], 1), jnp.concatenate([-pih, prh], 1)], 0
        )
        w_low[j] = jnp.concatenate(
            [jnp.concatenate([prl, pil], 1), jnp.concatenate([-pil, prl], 1)], 0
        )
        x_wave[j, 0] = re[24:]
        x_wave[j, 1] = im[24:]

    def multiply(j, half):
        q = jnp.int32(0)
        for end in ends[:7]:
            q = q + (end <= j).astype(jnp.int32)
        rows = pl.ds(half * HALF * 8, HALF * 8)
        high = gh[q, rows]
        top = w_high[j]
        return (
            jnp.dot(high, top, preferred_element_type=F32)
            + jnp.dot(gl[q, rows], top, preferred_element_type=F32)
            + jnp.dot(high, w_low[j], preferred_element_type=F32)
        )

    def finish(raw, j, half):
        xr, xi = x_wave[j, 0], x_wave[j, 1]
        re = raw[:, :128].reshape(HALF, 8, 128)
        im = raw[:, 128:].reshape(HALF, 8, 128)
        lanes = pl.ds(pl.multiple_of(j * 128, 128), 128)
        for part, value in enumerate((re * xr - im * xi, re * xi + im * xr)):
            first, rest = split(sum_over_x(value))
            yall[half, pl.ds(part * HALF, HALF), lanes] = first
            yall[half, pl.ds((2 + part) * HALF, HALF), lanes] = rest

    def four_tiles(i, half, ahead):
        out = [multiply(4 * i + k, half) for k in (0, 1)]
        for k in (2, 3):
            finish(raws[k], (4 * i + k + 2 * TILES - 2) % (TILES + 1), half)
        if ahead:
            prepare(4 * i + 4)
            prepare(4 * i + 5)
        for k in (0, 1):
            raws[k][...] = out[k]
        out = [multiply(4 * i + k, half) for k in (2, 3)]
        for k in (0, 1):
            finish(raws[k], 4 * i + k, half)
        if ahead:
            prepare(4 * i + 6)
            prepare(4 * i + 7)
        for k in (2, 3):
            raws[k][...] = out[k - 2]

    def tiles_loop(half):
        def step(i, carry):
            four_tiles(i, half, half == 0)
            return carry

        lax.fori_loop(0, 2, step, 0)

    def to_partner(half):
        return pltpu.make_async_remote_copy(
            src_ref=zbuf.at[half, 1 - core], dst_ref=dbuf.at[half],
            send_sem=pair_send.at[half], recv_sem=pair_recv.at[half],
            device_id=device((0, 0, 0), 1), device_id_type=MESH,
        )

    def restore(half):
        finish(raws[2], TILES - 1, half)
        back = jnp.dot(
            yall[half, :, : TILES * 128], pick[: TILES * 128], preferred_element_type=F32
        )
        back = back[: 2 * HALF] + back[2 * HALF :]
        fill = jnp.zeros((128 - HALF, 512), F32)
        for part in range(2):
            rows = jnp.concatenate([back[part * HALF : (part + 1) * HALF], fill], axis=0)
            zbuf[half, part] = jnp.transpose(rows)
        to_partner(half).start()

    def reduced(half):
        to_partner(half).wait_recv()
        total = (zbuf[half, core] + dbuf[half]) * (1.0 / math.sqrt(float(LX * LY * LZ * LT)))
        return total.reshape(64, 8, 128)

    def send_first():
        hbuf[...] = reduced(0)
        rbuf[chip] = hbuf[chip]
        for place in chips[:-1]:
            pltpu.make_async_remote_copy(
                src_ref=hbuf.at[chip_of(place)], dst_ref=rbuf.at[chip],
                send_sem=far_send.at[0], recv_sem=far_recv.at[0],
                device_id=device(place), device_id_type=MESH,
            ).start()

    def send_second():
        total = reduced(1)
        own_out[:, 0] = total[:, :4]
        own_out[:, 1] = total[:, 4:]
        own_in[core * 64 + chip] = own_out[chip, core]
        for place, dc in others:
            pltpu.make_async_remote_copy(
                src_ref=own_out.at[chip_of(place), cores[dc]],
                dst_ref=own_in.at[core * 64 + chip],
                send_sem=far_send.at[1], recv_sem=far_recv.at[1],
                device_id=device(place, dc), device_id_type=MESH,
            ).start()

    for k in range(4):
        prepare(jnp.int32(k))
    tiles_loop(0)
    four_tiles(2, 0, False)
    restore(0)
    tiles_loop(1)
    send_first()
    four_tiles(2, 1, False)
    restore(1)
    send_second()
    blocks = rbuf.at[pl.ds(0, 63)]
    owned = own_in.at[pl.ds(0, 127)]
    pltpu.make_async_copy(blocks, blocks, far_recv.at[0]).wait()
    spec[core, 0] = jnp.sum(rbuf[...], axis=0)
    last = pltpu.make_async_remote_copy(
        src_ref=spec.at[core, 0], dst_ref=spec.at[core, 0],
        send_sem=last_send, recv_sem=last_recv,
        device_id=device((0, 0, 0), 1), device_id_type=MESH,
    )
    last.start()
    pltpu.make_async_copy(all_rows, all_rows, mom_send).wait()
    for half in range(2):
        to_partner(half).wait_send()
    pltpu.make_async_copy(blocks, blocks, far_send.at[0]).wait()
    last.wait()
    pltpu.make_async_copy(owned, owned, far_recv.at[1]).wait()
    for part in range(2):
        mine = jnp.sum(own_in[part * 64 : part * 64 + 64], axis=0)
        spec[part, 1] = jnp.concatenate([mine, mine], axis=0)
    pltpu.make_async_copy(owned, owned, far_send.at[1]).wait()
    write_vertices(spec, widen, slots, out_ref)


def vertices_kernel_call(x, momenta, gamma_index):
    vmem = pl.BlockSpec(memory_space=pltpu.VMEM)
    dma = pltpu.SemaphoreType.DMA
    return pl.pallas_call(
        program_kernel,
        out_shape=pltpu.VMEM((4, 288, 16), F32),
        in_specs=[pl.BlockSpec(memory_space=pl.ANY)]
        + [pl.BlockSpec(memory_space=pltpu.SMEM)] * 2,
        out_specs=vmem,
        scratch_shapes=[
            pltpu.VMEM((144, 128, 128), F32),
            pltpu.VMEM((8, 1152, 256), BF16),
            pltpu.VMEM((8, 1152, 256), BF16),
            pltpu.VMEM((TILES + 1, 256, 256), BF16),
            pltpu.VMEM((TILES + 1, 256, 256), BF16),
            pltpu.VMEM((TILES + 1, 2, 8, 128), F32),
            *[pltpu.VMEM((HALF * 8, 256), F32)] * 4,
            pltpu.VMEM((2, 4 * HALF, (TILES + 1) * 128), BF16),
            pltpu.VMEM(((TILES + 1) * 128, 512), BF16),
            pltpu.VMEM((128, 1, 128), jnp.int32),
            pltpu.VMEM((512, 512), BF16),
            pltpu.VMEM((512, 512), BF16),
            pltpu.VMEM((256, 768), BF16),
            pltpu.VMEM((256, 512), BF16),
            pltpu.VMEM((2, 2, 512, 128), F32),
            pltpu.VMEM((2, 512, 128), F32),
            pltpu.VMEM((64, 8, 128), F32),
            pltpu.VMEM((64, 8, 128), F32),
            pltpu.VMEM((64, 2, 4, 128), F32),
            pltpu.VMEM((128, 4, 128), F32),
            pltpu.VMEM((2, 2, 8, 128), F32),
            dma((CHUNKS,)),
            dma, dma, dma((2,)), dma((2,)), dma((2,)), dma((2,)), dma, dma,
        ],
        compiler_params=pltpu.CompilerParams(
            collective_id=0, has_side_effects=True, vmem_limit_bytes=56 * 1024 * 1024
        ),
    )(x, momenta, gamma_index)


def site_major(propagator):
    x = jnp.transpose(propagator, (1, 2, 0, 3)).reshape(144, 2, 64, 128)
    return jnp.transpose(x, (0, 2, 1, 3)).reshape(144, 128, 128)


def body(propagator, momenta, gamma_index):
    out = vertices_kernel_call(site_major(propagator), momenta, gamma_index)
    return jnp.transpose(out.reshape(4, 12, 12, 2, 16), (0, 4, 3, 1, 2))


def solution(mesh):
    placed = (P(None, None, None, ("gx", "gz", "ta")), P(("gx", "gz", "ta"), None), P())
    return jax.shard_map(
        body,
        mesh=mesh,
        in_specs=placed,
        out_specs=P(("gx", "gz", "ta"), None, None, None, None),
        check_vma=False,
    )
```

```python
import math

import jax
import jax.numpy as jnp
import numpy as np
from jax import lax
from jax.experimental import pallas as pl
from jax.experimental.pallas import tpu as pltpu
from jax.sharding import PartitionSpec as P

LX = LY = LZ = LT = 32
MESH = pl.DeviceIdType.MESH
F32 = jnp.float32
BF16 = jnp.bfloat16
TILES = 11
CHUNKS = 18
HALF = 72


def split(value):
    high = value.astype(BF16)
    return high, (value - high.astype(F32)).astype(BF16)


def sine(index):
    turn = ((index + 16) & 31) - 16
    turn = jnp.where(turn > 8, 16 - turn, jnp.where(turn < -8, -16 - turn, turn))
    u = turn.astype(F32) * (math.pi / 16)
    s = u * u
    poly = 1 / 362880 - s * (1 / 39916800)
    for factor in (-1 / 5040, 1 / 120, -1 / 6, 1.0):
        poly = factor + s * poly
    return u * poly


def wave(index):
    return sine(index + 8), -sine(index)


def sum_over_x(value):
    groups = value.shape[0] // 8
    value = value.reshape(groups, 8, 8, 128)
    sub = lax.broadcasted_iota(jnp.int32, (8, 128), 0)
    for step in (4, 2, 1):
        keep = (sub & step) == 0
        out = []
        for k in range(step):
            a, b = value[:, k], value[:, k + step]
            rolled_a = pltpu.roll(a, 8 - step, 1)
            rolled_b = pltpu.roll(b, step, 1)
            out.append(jnp.where(keep, a, rolled_b) + jnp.where(keep, rolled_a, b))
        value = jnp.stack(out, axis=1)
    return value.reshape(groups * 8, 128)


NT = (((1,), (1,)), ((), ()))


def iota(shape, dim):
    return lax.broadcasted_iota(jnp.int32, shape, dim)


def fold_matrix():
    row, col = iota((128, 128), 0), iota((128, 128), 1)
    q = row >> 4
    number = jnp.where(q < 4, 2 * q, 2 * q - 7)
    re, im = wave(4 * number * ((col >> 1) & 7))
    from_im, to_im = (col & 1) == 1, ((row >> 3) & 1) == 1
    value = jnp.where(from_im == to_im, re, jnp.where(to_im, im, -im))
    return split(jnp.where((row & 7) == (col >> 4), value, 0.0))


def clifford_table():
    zeros = np.zeros((4, 4))
    first = (zeros, np.array([[0, 0, 0, 1], [0, 0, 1, 0], [0, -1, 0, 0], [-1, 0, 0, 0]]))
    second = (np.array([[0, 0, 0, -1], [0, 0, 1, 0], [0, 1, 0, 0], [-1, 0, 0, 0]]), zeros)
    third = (zeros, np.array([[0, 0, 1, 0], [0, 0, 0, -1], [-1, 0, 0, 0], [0, 1, 0, 0]]))
    fourth = (np.array([[0, 0, 1, 0], [0, 0, 0, 1], [1, 0, 0, 0], [0, 1, 0, 0]]), zeros)
    basis = [first, second, third, fourth]
    tables_re = []
    tables_im = []
    for mask in range(16):
        matrix_re = np.identity(4)
        matrix_im = np.zeros((4, 4))
        for bit in range(4):
            if mask >> bit & 1:
                basis_re, basis_im = basis[bit]
                new_re = matrix_re @ basis_re - matrix_im @ basis_im
                new_im = matrix_re @ basis_im + matrix_im @ basis_re
                matrix_re, matrix_im = (new_re, new_im)
        tables_re.append(matrix_re)
        tables_im.append(matrix_im)
    return (np.stack(tables_re), np.stack(tables_im))


def structures():
    table_re, table_im = clifford_table()
    out = []
    for re, im in zip(table_re, table_im, strict=True):
        matrix = im if im.any() else re
        columns = [int(np.flatnonzero(line)[0]) for line in matrix]
        signs = [float(line[k]) for line, k in zip(matrix, columns, strict=True)]
        out.append((bool(im.any()), columns, signs))
    return out


def widened(spec, widen, half):
    keep = iota((8, 128), 1) < HALF
    lines = []
    for k in range(6):
        for part in range(2):
            line = jnp.where(keep, spec[part, half], 0.0)
            lines.append(pltpu.roll(line, 128 - 12 * k, 1) if k else line)
    wide = jnp.concatenate(split(jnp.concatenate(lines, axis=0)), axis=1)
    wide = jnp.dot(wide, widen[...], preferred_element_type=F32)
    even = (iota((8, 384), 1) & 1) == 0
    out = []
    for k in range(6):
        left_re, re = wide[16 * k : 16 * k + 8, :384], wide[16 * k : 16 * k + 8, 384:]
        left_im, im = wide[16 * k + 8 : 16 * k + 16, :384], wide[16 * k + 8 : 16 * k + 16, 384:]
        out.append((left_re, left_im, jnp.where(even, re, im), jnp.where(even, im, -re)))
    return out


def write_vertices(sinks, slots, out_ref):
    even = (iota((8, 384), 1) & 1) == 0

    def pair(s, t):
        total = None
        for c in range(3):
            left_re, left_im = sinks[3 * s + c][:2]
            right, turned = sinks[3 * t + c][2:]
            term = left_re * right + left_im * turned
            total = term if total is None else total + term
        return total

    pairs = {}
    values = []
    for imaginary, columns, signs in structures():
        total = None
        for s in range(4):
            if (s, columns[s]) not in pairs:
                pairs[s, columns[s]] = pair(s, columns[s])
            term = pairs[s, columns[s]]
            if total is None:
                total = term if signs[s] > 0 else -term
            else:
                total = total + term if signs[s] > 0 else total - term
        if imaginary:
            total = jnp.where(even, -pltpu.roll(total, 383, 1), pltpu.roll(total, 1, 1))
        values.append(total)
    stacked = jnp.concatenate(split(jnp.concatenate(values, axis=0)), axis=0)
    out = lax.dot_general(
        stacked, slots[...], (((0,), (0,)), ((), ())), preferred_element_type=F32
    )
    for i in range(4):
        out_ref[i] = out[:288, i * 128 : i * 128 + 16]


def program_kernel(
    x_hbm, mom_smem, gamma_smem, out_ref,
    sbuf, gh, gl, w_high, w_low, x_wave, raw_a, raw_b, raw_c, raw_d, yall, pick, mom_all,
    before_buf, move_buf, widen, slots,
    zbuf, dbuf, hbuf, rbuf, own_out, own_in, spec,
    in_sems, mom_send, mom_recv, pair_send, pair_recv, far_send, far_recv, last_send, last_recv,
):
    gx, gz, ta = (lax.axis_index(name) for name in ("gx", "gz", "ta"))
    core, y_lo, z, y_hi = gz % 2, gz // 2, ta // 2, ta % 2
    y = y_hi * 2 + y_lo
    me = ((z * 4 + y) * 4 + gx) * 2 + core
    chip = (gx * 2 + y_lo) * 8 + ta
    xs = [gx] + [(gx + k) % 4 for k in range(1, 4)]
    ys = [y] + [(y + k) % 4 for k in range(1, 4)]
    zs = [z] + [(z + k) % 4 for k in range(1, 4)]
    cores = [core, 1 - core]
    gzs = [[(value % 2) * 2 + c for c in cores] for value in ys]
    tas = [[at_z * 2 + value // 2 for at_z in zs] for value in ys]
    hops = (0, 1, 2, 1)
    chips = sorted(
        ((dx, dy, dz) for dx in range(4) for dy in range(4) for dz in range(4)),
        key=lambda d: -sum(hops[k] for k in d),
    )

    def device(place, dc=0):
        dx, dy, dz = place
        return (xs[dx], gzs[dy][dc], tas[dy][dz])

    def chip_of(place):
        dx, dy, dz = place
        return (xs[dx] * 2 + ys[dy] % 2) * 8 + tas[dy][dz]

    raws = (raw_a, raw_b, raw_c, raw_d)
    barrier = pltpu.get_barrier_semaphore()
    others = [(place, dc) for place in chips for dc in (0, 1) if place != (0, 0, 0) or dc]
    for place, dc in others:
        pl.semaphore_signal(barrier, inc=1, device_id=device(place, dc), device_id_type=MESH)

    def load(k):
        part = pl.ds(k * 8, 8)
        return pltpu.make_async_copy(x_hbm.at[part], sbuf.at[part], in_sems.at[k])

    for k in range(CHUNKS):
        load(k).start()
    row = jnp.zeros((1, 128), jnp.int32)
    for i in range(4):
        for k in range(4):
            row = jnp.where(iota((1, 128), 1) == 4 * i + k, mom_smem[i, k], row)
    mom_all[me] = row

    fold_high, fold_low = fold_matrix()
    fold_twice = jnp.concatenate([fold_high, fold_high], axis=1)
    fold_rest = jnp.concatenate([fold_low, jnp.zeros_like(fold_low)], axis=1)[64:]

    def fold_step(k, carry):
        load(k).wait()
        for p in range(4):
            pair = k * 4 + p
            both = jnp.concatenate([sbuf[2 * pair], sbuf[2 * pair + 1]], axis=1)
            weights = jnp.concatenate(split(both), axis=0)
            out = jnp.dot(fold_twice, weights, preferred_element_type=F32)
            low = jnp.dot(fold_rest, weights, preferred_element_type=F32)
            out = jnp.concatenate([out[:64], out[64:] + low], axis=0)
            left = out[:, :128].reshape(16, 8, 128)
            right = out[:, 128:].reshape(16, 8, 128)
            high, rest = split(jnp.concatenate([left, right], axis=1))
            rows = pl.ds(pl.multiple_of(pair * 16, 16), 16)
            for q in range(8):
                for part in range(2):
                    lanes = slice(part * 128, part * 128 + 128)
                    gh[q, rows, lanes] = high[2 * q + part]
                    gl[q, rows, lanes] = rest[2 * q + part]
        return carry

    lax.fori_loop(0, 10, fold_step, 0)
    pl.semaphore_wait(barrier, 127)
    for place, dc in others:
        pltpu.make_async_remote_copy(
            src_ref=mom_all.at[me], dst_ref=mom_all.at[me], send_sem=mom_send, recv_sem=mom_recv,
            device_id=device(place, dc), device_id_type=MESH,
        ).start()
    lax.fori_loop(10, CHUNKS, fold_step, 0)

    before_buf[...] = (iota((512, 512), 0) < iota((512, 512), 1)).astype(F32).astype(BF16)
    to_row = iota((512, 512), 1)
    to_chip, to_core, own = to_row >> 3, (to_row >> 2) & 1, to_row & 3
    to_y = (to_chip & 1) * 2 + ((to_chip >> 3) & 1)
    source = own * 128 + ((to_chip >> 1) & 3) * 32 + to_y * 8 + (to_chip >> 4) * 2 + to_core
    move_buf[...] = (source == iota((512, 512), 0)).astype(F32).astype(BF16)
    lane = iota((128, 384), 1)
    source_a = (lane * 2731) >> 16
    source_b = (lane >> 1) - 12 * (((lane >> 1) * 5462) >> 16)
    for k, wanted in enumerate((source_a, source_b)):
        chosen = (iota((128, 384), 0) == wanted).astype(F32).astype(BF16)
        widen[:128, k * 384 : k * 384 + 384] = chosen
        widen[128:, k * 384 : k * 384 + 384] = chosen
    gamma_row = jnp.full((1, 128), -1, jnp.int32)
    for k in range(16):
        gamma_row = jnp.where(iota((1, 128), 1) == k, gamma_smem[k], gamma_row)
    row = iota((128, 128), 0)
    for i in range(4):
        chosen = ((row >> 3) == gamma_row) & ((row & 7) == core * 4 + i)
        chosen = chosen.astype(F32).astype(BF16)
        slots[:128, i * 128 : i * 128 + 128] = chosen
        slots[128:, i * 128 : i * 128 + 128] = chosen
    all_rows = mom_all.at[pl.ds(0, 127)]
    pltpu.make_async_copy(all_rows, all_rows, mom_recv).wait()

    turned = jnp.transpose((mom_all[...].reshape(128, 128) & 31).astype(F32))
    mom = jnp.concatenate([turned[4 * i : 4 * i + 4] for i in range(4)], axis=1)
    mom8 = jnp.concatenate([mom, jnp.zeros_like(mom)], axis=0).astype(BF16)
    mom8 = jnp.dot(mom8, move_buf[...], preferred_element_type=F32)
    ny = mom8[1:2].astype(jnp.int32)
    mom8 = mom8.astype(BF16)
    cls = ((ny >> 1) & 3) + 4 * (ny & 1)
    member = (iota((8, 512), 0) == cls).astype(F32)
    ahead = jnp.dot(member.astype(BF16), before_buf[...], preferred_element_type=F32)
    slot = jnp.sum(member * ahead, axis=0, keepdims=True)
    ends = []
    start = jnp.int32(0)
    for q in range(8):
        count = jnp.sum(member[q : q + 1]).astype(jnp.int32)
        slot = slot + member[q : q + 1] * (start * 128).astype(F32)
        start = start + ((count + 127) >> 7)
        ends.append(start)
    slot = slot.astype(jnp.int32)
    def prepare(j):
        here = (iota((128, 512), 0) + j * 128 == slot).astype(F32).astype(BF16)
        pick[pl.ds(pl.multiple_of(j * 128, 128), 128)] = here
        sorted_mom = lax.dot_general(mom8, here, NT, preferred_element_type=F32).astype(jnp.int32)
        nx, ny, nz, nt = (sorted_mom[i : i + 1] for i in range(4))
        k, r = iota((16, 128), 0), iota((8, 128), 0)
        phases = (
            nz * (r >> 2) + nt * (r & 3),
            ny * (k >> 2) + nz * (2 * (k & 3)),
            nx * (gx * 8 + r) + nz * (gz * 8) + nt * (ta * 4),
        )
        re, im = wave(jnp.concatenate(phases, axis=0))
        lr, li = re[:8], im[:8]
        rows = [(re[n : n + 1], im[n : n + 1]) for n in range(8, 24)]
        pr = jnp.concatenate([lr * hr - li * hi for hr, hi in rows], 0)
        pi = jnp.concatenate([lr * hi + li * hr for hr, hi in rows], 0)
        (prh, prl), (pih, pil) = split(pr), split(pi)
        w_high[j] = jnp.concatenate(
            [jnp.concatenate([prh, pih], 1), jnp.concatenate([-pih, prh], 1)], 0
        )
        w_low[j] = jnp.concatenate(
            [jnp.concatenate([prl, pil], 1), jnp.concatenate([-pil, prl], 1)], 0
        )
        x_wave[j, 0] = re[24:]
        x_wave[j, 1] = im[24:]

    def multiply(j, half):
        q = jnp.int32(0)
        for end in ends[:7]:
            q = q + (end <= j).astype(jnp.int32)
        rows = pl.ds(half * HALF * 8, HALF * 8)
        high = gh[q, rows]
        top = w_high[j]
        return (
            jnp.dot(high, top, preferred_element_type=F32)
            + jnp.dot(gl[q, rows], top, preferred_element_type=F32)
            + jnp.dot(high, w_low[j], preferred_element_type=F32)
        )

    def finish(raw, j, half):
        xr, xi = x_wave[j, 0], x_wave[j, 1]
        re = raw[:, :128].reshape(HALF, 8, 128)
        im = raw[:, 128:].reshape(HALF, 8, 128)
        lanes = pl.ds(pl.multiple_of(j * 128, 128), 128)
        for part, value in enumerate((re * xr - im * xi, re * xi + im * xr)):
            first, rest = split(sum_over_x(value))
            yall[half, pl.ds(part * HALF, HALF), lanes] = first
            yall[half, pl.ds((2 + part) * HALF, HALF), lanes] = rest

    def four_tiles(i, half, ahead):
        out = [multiply(4 * i + k, half) for k in (0, 1)]
        for k in (2, 3):
            finish(raws[k], (4 * i + k + 2 * TILES - 2) % (TILES + 1), half)
        if ahead:
            prepare(4 * i + 4)
            prepare(4 * i + 5)
        for k in (0, 1):
            raws[k][...] = out[k]
        out = [multiply(4 * i + k, half) for k in (2, 3)]
        for k in (0, 1):
            finish(raws[k], 4 * i + k, half)
        if ahead:
            prepare(4 * i + 6)
            prepare(4 * i + 7)
        for k in (2, 3):
            raws[k][...] = out[k - 2]

    def tiles_loop(half):
        def step(i, carry):
            four_tiles(i, half, half == 0)
            return carry

        lax.fori_loop(0, 2, step, 0)

    def to_partner(half):
        return pltpu.make_async_remote_copy(
            src_ref=zbuf.at[half, 1 - core], dst_ref=dbuf.at[half],
            send_sem=pair_send.at[half], recv_sem=pair_recv.at[half],
            device_id=device((0, 0, 0), 1), device_id_type=MESH,
        )

    def restore(half):
        finish(raws[2], TILES - 1, half)
        back = jnp.dot(
            yall[half, :, : TILES * 128], pick[: TILES * 128], preferred_element_type=F32
        )
        back = back[: 2 * HALF] + back[2 * HALF :]
        fill = jnp.zeros((128 - HALF, 512), F32)
        for part in range(2):
            rows = jnp.concatenate([back[part * HALF : (part + 1) * HALF], fill], axis=0)
            zbuf[half, part] = jnp.transpose(rows)
        to_partner(half).start()

    def reduced(half):
        to_partner(half).wait_recv()
        total = (zbuf[half, core] + dbuf[half]) * (1.0 / math.sqrt(float(LX * LY * LZ * LT)))
        return total.reshape(64, 8, 128)

    def send_first():
        hbuf[...] = reduced(0)
        rbuf[chip] = hbuf[chip]
        for place in chips[:-1]:
            pltpu.make_async_remote_copy(
                src_ref=hbuf.at[chip_of(place)], dst_ref=rbuf.at[chip],
                send_sem=far_send.at[0], recv_sem=far_recv.at[0],
                device_id=device(place), device_id_type=MESH,
            ).start()

    def send_second():
        total = reduced(1)
        own_out[:, 0] = total[:, :4]
        own_out[:, 1] = total[:, 4:]
        own_in[core * 64 + chip] = own_out[chip, core]
        for place, dc in others:
            pltpu.make_async_remote_copy(
                src_ref=own_out.at[chip_of(place), cores[dc]],
                dst_ref=own_in.at[core * 64 + chip],
                send_sem=far_send.at[1], recv_sem=far_recv.at[1],
                device_id=device(place, dc), device_id_type=MESH,
            ).start()

    for k in range(4):
        prepare(jnp.int32(k))
    tiles_loop(0)
    four_tiles(2, 0, False)
    restore(0)
    tiles_loop(1)
    send_first()
    four_tiles(2, 1, False)
    restore(1)
    send_second()
    blocks = rbuf.at[pl.ds(0, 63)]
    owned = own_in.at[pl.ds(0, 127)]
    pltpu.make_async_copy(blocks, blocks, far_recv.at[0]).wait()
    spec[core, 0] = jnp.sum(rbuf[...], axis=0)
    last = pltpu.make_async_remote_copy(
        src_ref=spec.at[core, 0], dst_ref=spec.at[core, 0],
        send_sem=last_send, recv_sem=last_recv,
        device_id=device((0, 0, 0), 1), device_id_type=MESH,
    )
    last.start()
    pltpu.make_async_copy(all_rows, all_rows, mom_send).wait()
    for half in range(2):
        to_partner(half).wait_send()
    pltpu.make_async_copy(blocks, blocks, far_send.at[0]).wait()
    last.wait()
    sinks = widened(spec, widen, 0)
    pltpu.make_async_copy(owned, owned, far_recv.at[1]).wait()
    for part in range(2):
        mine = jnp.sum(own_in[part * 64 : part * 64 + 64], axis=0)
        spec[part, 1] = jnp.concatenate([mine, mine], axis=0)
    pltpu.make_async_copy(owned, owned, far_send.at[1]).wait()
    write_vertices(sinks + widened(spec, widen, 1), slots, out_ref)


def vertices_kernel_call(x, momenta, gamma_index):
    vmem = pl.BlockSpec(memory_space=pltpu.VMEM)
    dma = pltpu.SemaphoreType.DMA
    return pl.pallas_call(
        program_kernel,
        out_shape=pltpu.VMEM((4, 288, 16), F32),
        in_specs=[pl.BlockSpec(memory_space=pl.ANY)]
        + [pl.BlockSpec(memory_space=pltpu.SMEM)] * 2,
        out_specs=vmem,
        scratch_shapes=[
            pltpu.VMEM((144, 128, 128), F32),
            pltpu.VMEM((8, 1152, 256), BF16),
            pltpu.VMEM((8, 1152, 256), BF16),
            pltpu.VMEM((TILES + 1, 256, 256), BF16),
            pltpu.VMEM((TILES + 1, 256, 256), BF16),
            pltpu.VMEM((TILES + 1, 2, 8, 128), F32),
            *[pltpu.VMEM((HALF * 8, 256), F32)] * 4,
            pltpu.VMEM((2, 4 * HALF, (TILES + 1) * 128), BF16),
            pltpu.VMEM(((TILES + 1) * 128, 512), BF16),
            pltpu.VMEM((128, 1, 128), jnp.int32),
            pltpu.VMEM((512, 512), BF16),
            pltpu.VMEM((512, 512), BF16),
            pltpu.VMEM((256, 768), BF16),
            pltpu.VMEM((256, 512), BF16),
            pltpu.VMEM((2, 2, 512, 128), F32),
            pltpu.VMEM((2, 512, 128), F32),
            pltpu.VMEM((64, 8, 128), F32),
            pltpu.VMEM((64, 8, 128), F32),
            pltpu.VMEM((64, 2, 4, 128), F32),
            pltpu.VMEM((128, 4, 128), F32),
            pltpu.VMEM((2, 2, 8, 128), F32),
            dma((CHUNKS,)),
            dma, dma, dma((2,)), dma((2,)), dma((2,)), dma((2,)), dma, dma,
        ],
        compiler_params=pltpu.CompilerParams(
            collective_id=0, has_side_effects=True, vmem_limit_bytes=56 * 1024 * 1024
        ),
    )(x, momenta, gamma_index)


def site_major(propagator):
    x = jnp.transpose(propagator, (1, 2, 0, 3)).reshape(144, 2, 64, 128)
    return jnp.transpose(x, (0, 2, 1, 3)).reshape(144, 128, 128)


def body(propagator, momenta, gamma_index):
    out = vertices_kernel_call(site_major(propagator), momenta, gamma_index)
    return jnp.transpose(out.reshape(4, 12, 12, 2, 16), (0, 4, 3, 1, 2))


def solution(mesh):
    placed = (P(None, None, None, ("gx", "gz", "ta")), P(("gx", "gz", "ta"), None), P())
    return jax.shard_map(
        body,
        mesh=mesh,
        in_specs=placed,
        out_specs=P(("gx", "gz", "ta"), None, None, None, None),
        check_vma=False,
    )
```

```python
import math

import jax
import jax.numpy as jnp
import numpy as np
from jax import lax
from jax.experimental import pallas as pl
from jax.experimental.pallas import tpu as pltpu
from jax.sharding import PartitionSpec as P

LX = LY = LZ = LT = 32
MESH = pl.DeviceIdType.MESH
F32 = jnp.float32
BF16 = jnp.bfloat16
TILES = 11
CHUNKS = 18
HALF = 72


def split(value):
    high = value.astype(BF16)
    return high, (value - high.astype(F32)).astype(BF16)


def sine(index):
    turn = ((index + 16) & 31) - 16
    turn = jnp.where(turn > 8, 16 - turn, jnp.where(turn < -8, -16 - turn, turn))
    u = turn.astype(F32) * (math.pi / 16)
    s = u * u
    poly = 1 / 362880 - s * (1 / 39916800)
    for factor in (-1 / 5040, 1 / 120, -1 / 6, 1.0):
        poly = factor + s * poly
    return u * poly


def wave(index):
    return sine(index + 8), -sine(index)


def sum_over_x(value):
    groups = value.shape[0] // 8
    value = value.reshape(groups, 8, 8, 128)
    sub = lax.broadcasted_iota(jnp.int32, (8, 128), 0)
    for step in (4, 2, 1):
        keep = (sub & step) == 0
        out = []
        for k in range(step):
            a, b = value[:, k], value[:, k + step]
            rolled_a = pltpu.roll(a, 8 - step, 1)
            rolled_b = pltpu.roll(b, step, 1)
            out.append(jnp.where(keep, a, rolled_b) + jnp.where(keep, rolled_a, b))
        value = jnp.stack(out, axis=1)
    return value.reshape(groups * 8, 128)


NT = (((1,), (1,)), ((), ()))


def iota(shape, dim):
    return lax.broadcasted_iota(jnp.int32, shape, dim)


def fold_matrix():
    row, col = iota((128, 128), 0), iota((128, 128), 1)
    q = row >> 4
    number = jnp.where(q < 4, 2 * q, 2 * q - 7)
    re, im = wave(4 * number * ((col >> 1) & 7))
    from_im, to_im = (col & 1) == 1, ((row >> 3) & 1) == 1
    value = jnp.where(from_im == to_im, re, jnp.where(to_im, im, -im))
    return split(jnp.where((row & 7) == (col >> 4), value, 0.0))


def clifford_table():
    zeros = np.zeros((4, 4))
    first = (zeros, np.array([[0, 0, 0, 1], [0, 0, 1, 0], [0, -1, 0, 0], [-1, 0, 0, 0]]))
    second = (np.array([[0, 0, 0, -1], [0, 0, 1, 0], [0, 1, 0, 0], [-1, 0, 0, 0]]), zeros)
    third = (zeros, np.array([[0, 0, 1, 0], [0, 0, 0, -1], [-1, 0, 0, 0], [0, 1, 0, 0]]))
    fourth = (np.array([[0, 0, 1, 0], [0, 0, 0, 1], [1, 0, 0, 0], [0, 1, 0, 0]]), zeros)
    basis = [first, second, third, fourth]
    tables_re = []
    tables_im = []
    for mask in range(16):
        matrix_re = np.identity(4)
        matrix_im = np.zeros((4, 4))
        for bit in range(4):
            if mask >> bit & 1:
                basis_re, basis_im = basis[bit]
                new_re = matrix_re @ basis_re - matrix_im @ basis_im
                new_im = matrix_re @ basis_im + matrix_im @ basis_re
                matrix_re, matrix_im = (new_re, new_im)
        tables_re.append(matrix_re)
        tables_im.append(matrix_im)
    return (np.stack(tables_re), np.stack(tables_im))


def structures():
    table_re, table_im = clifford_table()
    out = []
    for re, im in zip(table_re, table_im, strict=True):
        matrix = im if im.any() else re
        columns = [int(np.flatnonzero(line)[0]) for line in matrix]
        signs = [float(line[k]) for line, k in zip(matrix, columns, strict=True)]
        out.append((bool(im.any()), columns, signs))
    return out


def widened(spec, widen, half):
    keep = iota((8, 128), 1) < HALF
    lines = []
    for k in range(6):
        for part in range(2):
            line = jnp.where(keep, spec[part, half], 0.0)
            lines.append(pltpu.roll(line, 128 - 12 * k, 1) if k else line)
    wide = jnp.concatenate(split(jnp.concatenate(lines, axis=0)), axis=1)
    wide = jnp.dot(wide, widen[...], preferred_element_type=F32)
    even = (iota((8, 384), 1) & 1) == 0
    out = []
    for k in range(6):
        left_re, re = wide[16 * k : 16 * k + 8, :384], wide[16 * k : 16 * k + 8, 384:]
        left_im, im = wide[16 * k + 8 : 16 * k + 16, :384], wide[16 * k + 8 : 16 * k + 16, 384:]
        out.append((left_re, left_im, jnp.where(even, re, im), jnp.where(even, im, -re)))
    return out


def write_vertices(sinks, slots, out_ref):
    even = (iota((8, 384), 1) & 1) == 0

    def pair(s, t):
        total = None
        for c in range(3):
            left_re, left_im = sinks[3 * s + c][:2]
            right, turned = sinks[3 * t + c][2:]
            term = left_re * right + left_im * turned
            total = term if total is None else total + term
        return total

    pairs = {}
    values = []
    for imaginary, columns, signs in structures():
        total = None
        for s in range(4):
            if (s, columns[s]) not in pairs:
                pairs[s, columns[s]] = pair(s, columns[s])
            term = pairs[s, columns[s]]
            if total is None:
                total = term if signs[s] > 0 else -term
            else:
                total = total + term if signs[s] > 0 else total - term
        if imaginary:
            total = jnp.where(even, -pltpu.roll(total, 383, 1), pltpu.roll(total, 1, 1))
        values.append(total)
    stacked = jnp.concatenate(split(jnp.concatenate(values, axis=0)), axis=0)
    out = lax.dot_general(
        stacked, slots[...], (((0,), (0,)), ((), ())), preferred_element_type=F32
    )
    for i in range(4):
        out_ref[i] = out[:288, i * 128 : i * 128 + 16]


def program_kernel(
    x_hbm, mom_smem, gamma_smem, out_ref,
    sbuf, gh, gl, w_high, w_low, x_wave, raw_a, raw_b, raw_c, raw_d, yall, pick, mom_all,
    before_buf, move_buf, widen, slots,
    zbuf, dbuf, hbuf, rbuf, own_out, own_in, spec,
    in_sems, mom_send, mom_recv, pair_send, pair_recv, far_send, far_recv, last_send, last_recv,
):
    gx, gz, ta = (lax.axis_index(name) for name in ("gx", "gz", "ta"))
    core, y_lo, z, y_hi = gz % 2, gz // 2, ta // 2, ta % 2
    y = y_hi * 2 + y_lo
    me = ((z * 4 + y) * 4 + gx) * 2 + core
    chip = (gx * 2 + y_lo) * 8 + ta
    xs = [gx] + [(gx + k) % 4 for k in range(1, 4)]
    ys = [y] + [(y + k) % 4 for k in range(1, 4)]
    zs = [z] + [(z + k) % 4 for k in range(1, 4)]
    cores = [core, 1 - core]
    gzs = [[(value % 2) * 2 + c for c in cores] for value in ys]
    tas = [[at_z * 2 + value // 2 for at_z in zs] for value in ys]
    hops = (0, 1, 2, 1)
    chips = sorted(
        ((dx, dy, dz) for dx in range(4) for dy in range(4) for dz in range(4)),
        key=lambda d: -sum(hops[k] for k in d),
    )

    def device(place, dc=0):
        dx, dy, dz = place
        return (xs[dx], gzs[dy][dc], tas[dy][dz])

    def chip_of(place):
        dx, dy, dz = place
        return (xs[dx] * 2 + ys[dy] % 2) * 8 + tas[dy][dz]

    raws = (raw_a, raw_b, raw_c, raw_d)
    barrier = pltpu.get_barrier_semaphore()
    others = [(place, dc) for place in chips for dc in (0, 1) if place != (0, 0, 0) or dc]
    for place, dc in others:
        pl.semaphore_signal(barrier, inc=1, device_id=device(place, dc), device_id_type=MESH)

    def load(k):
        part = pl.ds(k * 8, 8)
        return pltpu.make_async_copy(x_hbm.at[part], sbuf.at[part], in_sems.at[k])

    for k in range(CHUNKS):
        load(k).start()
    row = jnp.zeros((1, 128), jnp.int32)
    for i in range(4):
        for k in range(4):
            row = jnp.where(iota((1, 128), 1) == 4 * i + k, mom_smem[i, k], row)
    mom_all[me] = row

    fold_high, fold_low = fold_matrix()
    fold_twice = jnp.concatenate([fold_high, fold_high], axis=1)
    fold_rest = jnp.concatenate([fold_low, jnp.zeros_like(fold_low)], axis=1)[64:]

    def fold_step(k, carry):
        load(k).wait()
        for p in range(4):
            pair = k * 4 + p
            both = jnp.concatenate([sbuf[2 * pair], sbuf[2 * pair + 1]], axis=1)
            weights = jnp.concatenate(split(both), axis=0)
            out = jnp.dot(fold_twice, weights, preferred_element_type=F32)
            low = jnp.dot(fold_rest, weights, preferred_element_type=F32)
            out = jnp.concatenate([out[:64], out[64:] + low], axis=0)
            left = out[:, :128].reshape(16, 8, 128)
            right = out[:, 128:].reshape(16, 8, 128)
            high, rest = split(jnp.concatenate([left, right], axis=1))
            rows = pl.ds(pl.multiple_of(pair * 16, 16), 16)
            for q in range(8):
                for part in range(2):
                    lanes = slice(part * 128, part * 128 + 128)
                    gh[q, rows, lanes] = high[2 * q + part]
                    gl[q, rows, lanes] = rest[2 * q + part]
        return carry

    lax.fori_loop(0, 5, fold_step, 0)
    pl.semaphore_wait(barrier, 127)
    for place, dc in others:
        pltpu.make_async_remote_copy(
            src_ref=mom_all.at[me], dst_ref=mom_all.at[me], send_sem=mom_send, recv_sem=mom_recv,
            device_id=device(place, dc), device_id_type=MESH,
        ).start()
    lax.fori_loop(5, CHUNKS, fold_step, 0)

    before_buf[...] = (iota((512, 512), 0) < iota((512, 512), 1)).astype(F32).astype(BF16)
    to_row = iota((512, 512), 1)
    to_chip, to_core, own = to_row >> 3, (to_row >> 2) & 1, to_row & 3
    to_y = (to_chip & 1) * 2 + ((to_chip >> 3) & 1)
    source = own * 128 + ((to_chip >> 1) & 3) * 32 + to_y * 8 + (to_chip >> 4) * 2 + to_core
    move_buf[...] = (source == iota((512, 512), 0)).astype(F32).astype(BF16)
    lane = iota((128, 384), 1)
    source_a = (lane * 2731) >> 16
    source_b = (lane >> 1) - 12 * (((lane >> 1) * 5462) >> 16)
    for k, wanted in enumerate((source_a, source_b)):
        chosen = (iota((128, 384), 0) == wanted).astype(F32).astype(BF16)
        widen[:128, k * 384 : k * 384 + 384] = chosen
        widen[128:, k * 384 : k * 384 + 384] = chosen
    gamma_row = jnp.full((1, 128), -1, jnp.int32)
    for k in range(16):
        gamma_row = jnp.where(iota((1, 128), 1) == k, gamma_smem[k], gamma_row)
    row = iota((128, 128), 0)
    for i in range(4):
        chosen = ((row >> 3) == gamma_row) & ((row & 7) == core * 4 + i)
        chosen = chosen.astype(F32).astype(BF16)
        slots[:128, i * 128 : i * 128 + 128] = chosen
        slots[128:, i * 128 : i * 128 + 128] = chosen
    all_rows = mom_all.at[pl.ds(0, 127)]
    pltpu.make_async_copy(all_rows, all_rows, mom_recv).wait()

    turned = jnp.transpose((mom_all[...].reshape(128, 128) & 31).astype(F32))
    mom = jnp.concatenate([turned[4 * i : 4 * i + 4] for i in range(4)], axis=1)
    mom8 = jnp.concatenate([mom, jnp.zeros_like(mom)], axis=0).astype(BF16)
    mom8 = jnp.dot(mom8, move_buf[...], preferred_element_type=F32)
    ny = mom8[1:2].astype(jnp.int32)
    mom8 = mom8.astype(BF16)
    cls = ((ny >> 1) & 3) + 4 * (ny & 1)
    member = (iota((8, 512), 0) == cls).astype(F32)
    ahead = jnp.dot(member.astype(BF16), before_buf[...], preferred_element_type=F32)
    slot = jnp.sum(member * ahead, axis=0, keepdims=True)
    ends = []
    start = jnp.int32(0)
    for q in range(8):
        count = jnp.sum(member[q : q + 1]).astype(jnp.int32)
        slot = slot + member[q : q + 1] * (start * 128).astype(F32)
        start = start + ((count + 127) >> 7)
        ends.append(start)
    slot = slot.astype(jnp.int32)
    def prepare(j):
        here = (iota((128, 512), 0) + j * 128 == slot).astype(F32).astype(BF16)
        pick[pl.ds(pl.multiple_of(j * 128, 128), 128)] = here
        sorted_mom = lax.dot_general(mom8, here, NT, preferred_element_type=F32).astype(jnp.int32)
        nx, ny, nz, nt = (sorted_mom[i : i + 1] for i in range(4))
        k, r = iota((16, 128), 0), iota((8, 128), 0)
        phases = (
            nz * (r >> 2) + nt * (r & 3),
            ny * (k >> 2) + nz * (2 * (k & 3)),
            nx * (gx * 8 + r) + nz * (gz * 8) + nt * (ta * 4),
        )
        re, im = wave(jnp.concatenate(phases, axis=0))
        lr, li = re[:8], im[:8]
        rows = [(re[n : n + 1], im[n : n + 1]) for n in range(8, 24)]
        pr = jnp.concatenate([lr * hr - li * hi for hr, hi in rows], 0)
        pi = jnp.concatenate([lr * hi + li * hr for hr, hi in rows], 0)
        (prh, prl), (pih, pil) = split(pr), split(pi)
        w_high[j] = jnp.concatenate(
            [jnp.concatenate([prh, pih], 1), jnp.concatenate([-pih, prh], 1)], 0
        )
        w_low[j] = jnp.concatenate(
            [jnp.concatenate([prl, pil], 1), jnp.concatenate([-pil, prl], 1)], 0
        )
        x_wave[j, 0] = re[24:]
        x_wave[j, 1] = im[24:]

    def multiply(j, half):
        q = jnp.int32(0)
        for end in ends[:7]:
            q = q + (end <= j).astype(jnp.int32)
        rows = pl.ds(half * HALF * 8, HALF * 8)
        high = gh[q, rows]
        top = w_high[j]
        return (
            jnp.dot(high, top, preferred_element_type=F32)
            + jnp.dot(gl[q, rows], top, preferred_element_type=F32)
            + jnp.dot(high, w_low[j], preferred_element_type=F32)
        )

    def finish(raw, j, half):
        xr, xi = x_wave[j, 0], x_wave[j, 1]
        re = raw[:, :128].reshape(HALF, 8, 128)
        im = raw[:, 128:].reshape(HALF, 8, 128)
        lanes = pl.ds(pl.multiple_of(j * 128, 128), 128)
        for part, value in enumerate((re * xr - im * xi, re * xi + im * xr)):
            first, rest = split(sum_over_x(value))
            yall[half, pl.ds(part * HALF, HALF), lanes] = first
            yall[half, pl.ds((2 + part) * HALF, HALF), lanes] = rest

    def four_tiles(i, half, ahead):
        out = [multiply(4 * i + k, half) for k in (0, 1)]
        for k in (2, 3):
            finish(raws[k], (4 * i + k + 2 * TILES - 2) % (TILES + 1), half)
        if ahead:
            prepare(4 * i + 4)
            prepare(4 * i + 5)
        for k in (0, 1):
            raws[k][...] = out[k]
        out = [multiply(4 * i + k, half) for k in (2, 3)]
        for k in (0, 1):
            finish(raws[k], 4 * i + k, half)
        if ahead:
            prepare(4 * i + 6)
            prepare(4 * i + 7)
        for k in (2, 3):
            raws[k][...] = out[k - 2]

    def tiles_loop(half):
        def step(i, carry):
            four_tiles(i, half, half == 0)
            return carry

        lax.fori_loop(0, 2, step, 0)

    def to_partner(half):
        return pltpu.make_async_remote_copy(
            src_ref=zbuf.at[half, 1 - core], dst_ref=dbuf.at[half],
            send_sem=pair_send.at[half], recv_sem=pair_recv.at[half],
            device_id=device((0, 0, 0), 1), device_id_type=MESH,
        )

    def restore(half):
        finish(raws[2], TILES - 1, half)
        back = jnp.dot(
            yall[half, :, : TILES * 128], pick[: TILES * 128], preferred_element_type=F32
        )
        back = back[: 2 * HALF] + back[2 * HALF :]
        fill = jnp.zeros((128 - HALF, 512), F32)
        for part in range(2):
            rows = jnp.concatenate([back[part * HALF : (part + 1) * HALF], fill], axis=0)
            zbuf[half, part] = jnp.transpose(rows)
        to_partner(half).start()

    def reduced(half):
        to_partner(half).wait_recv()
        total = (zbuf[half, core] + dbuf[half]) * (1.0 / math.sqrt(float(LX * LY * LZ * LT)))
        return total.reshape(64, 8, 128)

    def send_first():
        hbuf[...] = reduced(0)
        rbuf[chip] = hbuf[chip]
        for place in chips[:-1]:
            pltpu.make_async_remote_copy(
                src_ref=hbuf.at[chip_of(place)], dst_ref=rbuf.at[chip],
                send_sem=far_send.at[0], recv_sem=far_recv.at[0],
                device_id=device(place), device_id_type=MESH,
            ).start()

    def send_second():
        total = reduced(1)
        own_out[:, 0] = total[:, :4]
        own_out[:, 1] = total[:, 4:]
        own_in[core * 64 + chip] = own_out[chip, core]
        for place, dc in others:
            pltpu.make_async_remote_copy(
                src_ref=own_out.at[chip_of(place), cores[dc]],
                dst_ref=own_in.at[core * 64 + chip],
                send_sem=far_send.at[1], recv_sem=far_recv.at[1],
                device_id=device(place, dc), device_id_type=MESH,
            ).start()

    for k in range(4):
        prepare(jnp.int32(k))
    tiles_loop(0)
    four_tiles(2, 0, False)
    restore(0)
    tiles_loop(1)
    send_first()
    four_tiles(2, 1, False)
    restore(1)
    send_second()
    blocks = rbuf.at[pl.ds(0, 63)]
    owned = own_in.at[pl.ds(0, 127)]
    pltpu.make_async_copy(blocks, blocks, far_recv.at[0]).wait()
    spec[core, 0] = jnp.sum(rbuf[...], axis=0)
    last = pltpu.make_async_remote_copy(
        src_ref=spec.at[core, 0], dst_ref=spec.at[core, 0],
        send_sem=last_send, recv_sem=last_recv,
        device_id=device((0, 0, 0), 1), device_id_type=MESH,
    )
    last.start()
    pltpu.make_async_copy(all_rows, all_rows, mom_send).wait()
    for half in range(2):
        to_partner(half).wait_send()
    pltpu.make_async_copy(blocks, blocks, far_send.at[0]).wait()
    last.wait()
    sinks = widened(spec, widen, 0)
    pltpu.make_async_copy(owned, owned, far_recv.at[1]).wait()
    for part in range(2):
        mine = jnp.sum(own_in[part * 64 : part * 64 + 64], axis=0)
        spec[part, 1] = jnp.concatenate([mine, mine], axis=0)
    pltpu.make_async_copy(owned, owned, far_send.at[1]).wait()
    write_vertices(sinks + widened(spec, widen, 1), slots, out_ref)


def vertices_kernel_call(x, momenta, gamma_index):
    vmem = pl.BlockSpec(memory_space=pltpu.VMEM)
    dma = pltpu.SemaphoreType.DMA
    return pl.pallas_call(
        program_kernel,
        out_shape=pltpu.VMEM((4, 288, 16), F32),
        in_specs=[pl.BlockSpec(memory_space=pl.ANY)]
        + [pl.BlockSpec(memory_space=pltpu.SMEM)] * 2,
        out_specs=vmem,
        scratch_shapes=[
            pltpu.VMEM((144, 128, 128), F32),
            pltpu.VMEM((8, 1152, 256), BF16),
            pltpu.VMEM((8, 1152, 256), BF16),
            pltpu.VMEM((TILES + 1, 256, 256), BF16),
            pltpu.VMEM((TILES + 1, 256, 256), BF16),
            pltpu.VMEM((TILES + 1, 2, 8, 128), F32),
            *[pltpu.VMEM((HALF * 8, 256), F32)] * 4,
            pltpu.VMEM((2, 4 * HALF, (TILES + 1) * 128), BF16),
            pltpu.VMEM(((TILES + 1) * 128, 512), BF16),
            pltpu.VMEM((128, 1, 128), jnp.int32),
            pltpu.VMEM((512, 512), BF16),
            pltpu.VMEM((512, 512), BF16),
            pltpu.VMEM((256, 768), BF16),
            pltpu.VMEM((256, 512), BF16),
            pltpu.VMEM((2, 2, 512, 128), F32),
            pltpu.VMEM((2, 512, 128), F32),
            pltpu.VMEM((64, 8, 128), F32),
            pltpu.VMEM((64, 8, 128), F32),
            pltpu.VMEM((64, 2, 4, 128), F32),
            pltpu.VMEM((128, 4, 128), F32),
            pltpu.VMEM((2, 2, 8, 128), F32),
            dma((CHUNKS,)),
            dma, dma, dma((2,)), dma((2,)), dma((2,)), dma((2,)), dma, dma,
        ],
        compiler_params=pltpu.CompilerParams(
            collective_id=0, has_side_effects=True, vmem_limit_bytes=56 * 1024 * 1024
        ),
    )(x, momenta, gamma_index)


def site_major(propagator):
    x = jnp.transpose(propagator, (1, 2, 0, 3)).reshape(144, 2, 64, 128)
    return jnp.transpose(x, (0, 2, 1, 3)).reshape(144, 128, 128)


def body(propagator, momenta, gamma_index):
    out = vertices_kernel_call(site_major(propagator), momenta, gamma_index)
    return jnp.transpose(out.reshape(4, 12, 12, 2, 16), (0, 4, 3, 1, 2))


def solution(mesh):
    placed = (P(None, None, None, ("gx", "gz", "ta")), P(("gx", "gz", "ta"), None), P())
    return jax.shard_map(
        body,
        mesh=mesh,
        in_specs=placed,
        out_specs=P(("gx", "gz", "ta"), None, None, None, None),
        check_vma=False,
    )
```
